32 devices in a mesh: twin: 2 (over x), dp: 16 (over z, y, core).
Axes of the slice: x: 2, y: 2, z: 4, core: 2. Of those that a mesh axis runs over, the one named last changes fastest.
Arguments:
- hidden_in: bfloat16 [2, 32, 512, 768], P('twin', 'dp'), may hold values from -6 to 6
- seq_lengths: int32 [2, 32], P('twin', 'dp'), may hold values from 64 to 512, as said below
- pos_index: int32 [2, 16, 6], replicated, may hold values from 0 to 15
- pos_count: int32 [2, 16], replicated, may hold values from 1 to 6, as said below
- query_proj: float32 [768, 768], P(('twin', 'dp')), may hold values from -0.21875 to 0.21875
- key_proj: float32 [768, 768], P(('twin', 'dp')), may hold values from -0.21875 to 0.21875
- value_proj: float32 [768, 768], P(('twin', 'dp')), may hold values from -0.21875 to 0.21875
- mixer_proj: float32 [768, 768], P(('twin', 'dp')), may hold values from -3 to 3
- expand_proj: float32 [768, 3072], P(('twin', 'dp')), may hold values from -0.21875 to 0.21875
- shrink_proj: float32 [3072, 768], P(('twin', 'dp')), may hold values from -0.109375 to 0.109375
- query_bias: float32 [768], P(('twin', 'dp')), may hold values from -1 to 1
- value_bias: float32 [768], P(('twin', 'dp')), may hold values from -1 to 1
- mixer_bias: float32 [768], P(('twin', 'dp')), may hold values from -1 to 1
- first_gain: float32 [768], P(('twin', 'dp')), may hold values from 0.5 to 1.5
- first_shift: float32 [768], P(('twin', 'dp')), may hold values from -1 to 1
- expand_bias: float32 [3072], P(('twin', 'dp')), may hold values from -1 to 1
- shrink_bias: float32 [768], P(('twin', 'dp')), may hold values from -1 to 1
- second_gain: float32 [768], P(('twin', 'dp')), may hold values from 0.5 to 1.5
- second_shift: float32 [768], P(('twin', 'dp')), may hold values from -0.3 to 0.3
Outputs:
- loss_value: float32 [], replicated
- hidden_grad: float32 [2, 32, 512, 768], P('twin', 'dp')
- queryproj_grad: float32 [768, 768], P(('twin', 'dp'))
- keyproj_grad: float32 [768, 768], P(('twin', 'dp'))
- valueproj_grad: float32 [768, 768], P(('twin', 'dp'))
- mixerproj_grad: float32 [768, 768], P(('twin', 'dp'))
- expandproj_grad: float32 [768, 3072], P(('twin', 'dp'))
- shrinkproj_grad: float32 [3072, 768], P(('twin', 'dp'))
- querybias_grad: float32 [768], P(('twin', 'dp'))
- valuebias_grad: float32 [768], P(('twin', 'dp'))
- mixerbias_grad: float32 [768], P(('twin', 'dp'))
- firstgain_grad: float32 [768], P(('twin', 'dp'))
- firstshift_grad: float32 [768], P(('twin', 'dp'))
- expandbias_grad: float32 [3072], P(('twin', 'dp'))
- shrinkbias_grad: float32 [768], P(('twin', 'dp'))
- secondgain_grad: float32 [768], P(('twin', 'dp'))
- secondshift_grad: float32 [768], P(('twin', 'dp'))
The draws below stay inside these ranges and needn't reach their ends.
Inputs may be any that keep to these rules, and one draw needn't show every extreme that they name: `seq_lengths`: each sentence's valid tokens come first; some sentence has 512 and some has 64. Only the first pos_count entries of an anchor's list count; counts are heavy-tailed and both ends occur in every micro-batch. `pos_index`: a list may name a paraphrase more than once; each naming counts.
All inputs are finite; a program needn't handle non-finite values.
Results may differ from the reference program's by a relative error of at most 0.014.
Values may be sent and summed in bfloat16 or wider, within the bound.
A program may use at most 192 MiB of HBM per device.

```python
from functools import partial
import jax
import jax.numpy as jnp
from jax import lax

D = 768
HEADS = 12
HDIM = 64
FF = 3072
LEN = 512
MICRO = 2
KMAX = 6
SEQ_MB = 1
ANCH = 16
SEQS = 32
N_DP = 16


def draw_seq_lengths(key, part):
    drawn = jax.random.randint(key, (2, SEQS), LEN // 8, LEN + 1)
    drawn = drawn.at[:, 0].set(LEN)
    return drawn.at[:, 1].set(LEN // 8)


def draw_pos_count(key, part):
    picks = jax.random.randint(key, (MICRO, ANCH), 0, 64)
    counts = 1 + (picks >= 32).astype(jnp.int32) + (picks >= 48).astype(jnp.int32) + (picks >= 56).astype(jnp.int32) + (picks >= 60).astype(jnp.int32) + (picks >= 62).astype(jnp.int32)
    counts = counts.at[:, 0].set(KMAX)
    return counts.at[:, 1].set(1)


def set_ends(values, key, smallest, top_value):
    shape = values.shape
    index_at = [jax.random.randint(jax.random.fold_in(key, axis), (), 0, shape[axis]) for axis in range(len(shape))]
    values = values.at[tuple(index_at)].set(smallest)
    longest = shape.index(max(shape))
    index_at[longest] = (index_at[longest] + 1) % shape[longest]
    return values.at[tuple(index_at)].set(top_value)


def levels(own_key, shape, cuts, least, high):
    def one(position, parts):
        steps = jax.random.uniform(jax.random.fold_in(jax.random.fold_in(own_key, 6), position), (parts,), jnp.float32, least / len(cuts), high / len(cuts))
        return jnp.repeat(jnp.exp(steps), shape[position] // parts).reshape((-1,) + (1,) * (len(shape) - position - 1))

    factor_of = one(*cuts[0])
    for cut in cuts[1:]:
        factor_of = factor_of * one(*cut)
    return factor_of


def noise(stream_key, dims, scale, bound, shards=(), held_as=jnp.bfloat16):
    values = scale * jax.random.normal(stream_key, dims, jnp.float32)
    if shards:
        values = values * levels(stream_key, dims, shards, -0.22, 0.18)
    return jnp.clip(values, -bound, bound).astype(held_as)


def setup_inputs(seed: int = 0) -> dict:
    key_list = jax.random.split(jax.random.key(seed), 20)
    return {
        "hidden_in": noise(key_list[0], (2, SEQS, LEN, D), 1.0, 6.0, ((0, 2), (1, 16))),
        "seq_lengths": draw_seq_lengths(jax.random.fold_in(key_list[19], 71), 0),
        "pos_index": set_ends(jax.random.randint(key_list[2], (MICRO, ANCH, KMAX), 0, ANCH), jax.random.fold_in(key_list[2], 1), 0, ANCH - 1).astype(jnp.int32),
        "pos_count": draw_pos_count(jax.random.fold_in(key_list[19], 71), 0),
        "query_proj": noise(key_list[4], (D, D), D ** -0.5, 0.21875, ((0, 32),), jnp.float32),
        "key_proj": noise(key_list[5], (D, D), D ** -0.5, 0.21875, ((0, 32),), jnp.float32),
        "value_proj": noise(key_list[6], (D, D), D ** -0.5, 0.21875, ((0, 32),), jnp.float32),
        "mixer_proj": noise(key_list[7], (D, D), (max(D * 3 // LEN, 1)) ** -0.5, 3.0, ((0, 32),), jnp.float32),
        "expand_proj": noise(key_list[8], (D, FF), D ** -0.5, 0.21875, ((0, 32),), jnp.float32),
        "shrink_proj": noise(key_list[9], (FF, D), FF ** -0.5, 0.109375, ((0, 32),), jnp.float32),
        "query_bias": noise(key_list[10], (D,), 0.2, 1.0, ((0, 32),), jnp.float32),
        "value_bias": noise(key_list[11], (D,), 0.2, 1.0, ((0, 32),), jnp.float32),
        "mixer_bias": noise(key_list[12], (D,), 0.2, 1.0, ((0, 32),), jnp.float32),
        "first_gain": jnp.clip(1.0 + 0.1 * jax.random.normal(key_list[13], (D,), jnp.float32), 0.5, 1.5),
        "first_shift": noise(key_list[14], (D,), 0.2, 1.0, ((0, 32),), jnp.float32),
        "expand_bias": noise(key_list[15], (FF,), 0.2, 1.0, ((0, 32),), jnp.float32),
        "shrink_bias": noise(key_list[16], (D,), 0.2, 1.0, ((0, 32),), jnp.float32),
        "second_gain": jnp.clip(1.0 + 0.1 * jax.random.normal(key_list[17], (D,), jnp.float32), 0.5, 1.5),
        "second_shift": noise(key_list[18], (D,), 0.05, 0.3, ((0, 32),), jnp.float32),
    }


norm_eps = 1e-12
cosine_scale = 50.0
static_scale = 256.0

@jax.custom_vjp
def low(v):
    return lax.optimization_barrier(v.astype(jnp.bfloat16)).astype(jnp.float32)

@jax.custom_vjp
def low_back(v):
    return v

def low_keep(v):
    return (low(v), None)

def low_pass(kept, grad):
    return (grad,)

def back_keep(v):
    return (v, None)

def back_low(kept, grad):
    return (low(grad),)
low.defvjp(low_keep, low_pass)
low_back.defvjp(back_keep, back_low)

def round_both(values):
    return low_back(low(values))

def product(left, right):
    return jnp.dot(left, right, precision=lax.Precision.HIGHEST)

def layer_norm(values, gain_vec, shift_vec):
    center = values - lax.optimization_barrier(jnp.mean(values, axis=-1, keepdims=True))
    spread = lax.optimization_barrier(jnp.mean(center * center, axis=-1, keepdims=True))
    return center * lax.rsqrt(spread + norm_eps) * gain_vec + shift_vec

def encode(tokens, length, params):
    live_mask = jnp.arange(LEN, dtype=jnp.int32) < length
    head_shape = (LEN, HEADS, HDIM)
    query = round_both(product(tokens, params[0]) + params[6]).reshape(head_shape)
    keys_all = round_both(product(tokens, params[1])).reshape(head_shape)
    values_all = round_both(product(tokens, params[2]) + params[7]).reshape(head_shape)
    raw_scores = jnp.einsum('qhd,khd->hqk', query, keys_all, precision=lax.Precision.HIGHEST)
    scores = low_back(raw_scores * HDIM ** (-0.5))
    scores = jnp.where(live_mask[None, None, :], scores, -1000000000.0)
    row_top = lax.optimization_barrier(jnp.max(scores, axis=-1, keepdims=True))
    exp_terms = jnp.exp(scores - row_top)
    probs_low = low(exp_terms / lax.optimization_barrier(jnp.sum(exp_terms, axis=-1, keepdims=True)))
    mixed = jnp.einsum('hqk,khd->qhd', probs_low, values_all, precision=lax.Precision.HIGHEST)
    mixed = round_both(mixed.reshape(LEN, D))
    branch = low_back(product(mixed, params[3]) + params[8])
    normed = layer_norm(tokens + branch, params[9], params[10])
    inner = low_back(product(low(normed), params[4]) + params[11])
    active = low(jax.nn.gelu(inner, approximate=False))
    ffn_out = low_back(product(active, params[5]) + params[12])
    output = layer_norm(normed + ffn_out, params[13], params[14])
    pool_weight = live_mask.astype(jnp.float32) / length.astype(jnp.float32)
    return low(lax.optimization_barrier(jnp.sum(output * pool_weight[:, None], axis=0)))

def batch_loss(pooled_all, pos_list, pos_num):
    anchors = pooled_all.shape[0] // 2
    anchor = pooled_all[:anchors]
    positive = pooled_all[anchors:]
    anchor_n = anchor * lax.rsqrt(lax.optimization_barrier(jnp.sum(anchor * anchor, axis=-1, keepdims=True)) + 1e-06)
    positive_n = positive * lax.rsqrt(lax.optimization_barrier(jnp.sum(positive * positive, axis=-1, keepdims=True)) + 1e-06)
    sims = cosine_scale * jnp.dot(anchor_n, positive_n.T, precision=lax.Precision.HIGHEST)
    row_top = lax.optimization_barrier(jnp.max(sims, axis=-1, keepdims=True))
    log_total = row_top[:, 0] + jnp.log(lax.optimization_barrier(jnp.sum(jnp.exp(sims - row_top), axis=-1)))
    columns = jnp.arange(anchors, dtype=jnp.int32)
    slots = jnp.arange(pos_list.shape[1], dtype=jnp.int32)
    hits = (pos_list[:, :, None] == columns[None, None, :]) & (slots[None, :, None] < pos_num[:, None, None])
    target = lax.optimization_barrier(jnp.sum(hits.astype(jnp.float32), axis=1)) / pos_num[:, None].astype(jnp.float32)
    return jnp.sum(log_total - lax.optimization_barrier(jnp.sum(target * sims, axis=-1)))

def reference(hidden_in, seq_lengths, pos_index, pos_count, query_proj, key_proj, value_proj, mixer_proj, expand_proj, shrink_proj, query_bias, value_bias, mixer_bias, first_gain, first_shift, expand_bias, shrink_bias, second_gain, second_shift):
    masters = (query_proj, key_proj, value_proj, mixer_proj, expand_proj, shrink_proj, query_bias, value_bias, mixer_bias, first_gain, first_shift, expand_bias, shrink_bias, second_gain, second_shift)
    anchors = SEQ_MB * N_DP
    lengths_all = seq_lengths.reshape(2, N_DP, MICRO, SEQ_MB).transpose(2, 0, 1, 3).reshape(MICRO * 2 * anchors)

    def objective(tokens_in, weights):
        params = tuple((low(item) for item in weights))
        sentences = tokens_in.reshape(2, N_DP, MICRO, SEQ_MB, LEN, D).transpose(2, 0, 1, 3, 4, 5)
        sentences = sentences.reshape(MICRO * 2 * anchors, LEN, D)
        encoder = jax.checkpoint(partial(encode, params=params))
        pooled = lax.map(lambda pair: encoder(pair[0], pair[1]), (sentences, lengths_all))
        pooled = pooled.reshape(MICRO, 2 * anchors, D)
        total = jnp.zeros((), jnp.float32)
        for micro_step in range(MICRO):
            total = total + batch_loss(pooled[micro_step], pos_index[micro_step], pos_count[micro_step])
        return (static_scale * total, total)
    scaled, pull, raw_total = jax.vjp(objective, hidden_in.astype(jnp.float32), masters, has_aux=True)
    grad_tokens, grad_weights = pull(jnp.ones((), jnp.float32))
    return (raw_total / (MICRO * anchors), grad_tokens, grad_weights[0], grad_weights[1], grad_weights[2], grad_weights[3], grad_weights[4], grad_weights[5], grad_weights[6], grad_weights[7], grad_weights[8], grad_weights[9], grad_weights[10], grad_weights[11], grad_weights[12], grad_weights[13], grad_weights[14])
```

```python
import jax
import jax.numpy as jnp
from jax import lax
from jax.experimental import pallas as pl
from jax.experimental.pallas import tpu as pltpu
from jax.sharding import PartitionSpec as P

HEADS = 12
HDIM = 64
MICRO = 2


norm_eps = 1e-12
cosine_scale = 50.0
static_scale = 256.0


def layer_norm(values, gain_vec, shift_vec):
    center = values - jnp.mean(values, axis=-1, keepdims=True)
    spread = jnp.mean(center * center, axis=-1, keepdims=True)
    return center * lax.rsqrt(spread + norm_eps) * gain_vec + shift_vec


def exact_gelu(values):
    return jax.nn.gelu(values, approximate=False)


def product(left, right):
    return jnp.dot(left, right, preferred_element_type=jnp.float32)


def product_lt(left, right):
    return lax.dot_general(
        left, right, (((0,), (0,)), ((), ())), preferred_element_type=jnp.float32
    )


def product_rt(left, right):
    return lax.dot_general(
        left, right, (((1,), (1,)), ((), ())), preferred_element_type=jnp.float32
    )


def column_sum(values):
    return jnp.sum(values.astype(jnp.float32), axis=0)


def batch_loss(pooled_all, pos_list, pos_num):
    anchors = pooled_all.shape[0] // 2
    anchor = pooled_all[:anchors]
    positive = pooled_all[anchors:]
    anchor_n = anchor * lax.rsqrt(jnp.sum(anchor * anchor, axis=-1, keepdims=True) + 1e-06)
    positive_n = positive * lax.rsqrt(jnp.sum(positive * positive, axis=-1, keepdims=True) + 1e-06)
    sims = cosine_scale * jnp.dot(anchor_n, positive_n.T, precision=lax.Precision.HIGHEST)
    row_top = jnp.max(sims, axis=-1, keepdims=True)
    log_total = row_top[:, 0] + jnp.log(jnp.sum(jnp.exp(sims - row_top), axis=-1))
    columns = jnp.arange(anchors, dtype=jnp.int32)
    slots = jnp.arange(pos_list.shape[1], dtype=jnp.int32)
    hits = (pos_list[:, :, None] == columns[None, None, :]) & (
        slots[None, :, None] < pos_num[:, None, None]
    )
    target = jnp.sum(hits.astype(jnp.float32), axis=1) / pos_num[:, None].astype(jnp.float32)
    return jnp.sum(log_total - jnp.sum(target * sims, axis=-1))


def fetch_weights(masters):
    return (
        lax.all_gather(masters[0].astype(jnp.bfloat16), ("twin", "dp"), axis=0, tiled=True),
        lax.all_gather(masters[1].astype(jnp.bfloat16), ("twin", "dp"), axis=0, tiled=True),
        lax.all_gather(masters[2].astype(jnp.bfloat16), ("twin", "dp"), axis=0, tiled=True),
        lax.all_gather(masters[3].astype(jnp.bfloat16), ("twin", "dp"), axis=0, tiled=True),
        lax.all_gather(masters[4].astype(jnp.bfloat16), ("twin", "dp"), axis=0, tiled=True),
        lax.all_gather(masters[5].astype(jnp.bfloat16), ("twin", "dp"), axis=0, tiled=True),
        lax.all_gather(masters[6].astype(jnp.bfloat16), ("twin", "dp"), axis=0, tiled=True),
        lax.all_gather(masters[7].astype(jnp.bfloat16), ("twin", "dp"), axis=0, tiled=True),
        lax.all_gather(masters[8].astype(jnp.bfloat16), ("twin", "dp"), axis=0, tiled=True),
        lax.all_gather(masters[9].astype(jnp.bfloat16), ("twin", "dp"), axis=0, tiled=True),
        lax.all_gather(masters[10].astype(jnp.bfloat16), ("twin", "dp"), axis=0, tiled=True),
        lax.all_gather(masters[11].astype(jnp.bfloat16), ("twin", "dp"), axis=0, tiled=True),
        lax.all_gather(masters[12].astype(jnp.bfloat16), ("twin", "dp"), axis=0, tiled=True),
        lax.all_gather(masters[13].astype(jnp.bfloat16), ("twin", "dp"), axis=0, tiled=True),
        lax.all_gather(masters[14].astype(jnp.bfloat16), ("twin", "dp"), axis=0, tiled=True),
    )


def settle_grads(grad_sums):
    return (
        lax.psum_scatter(grad_sums[0], ("twin", "dp"), scatter_dimension=0, tiled=True),
        lax.psum_scatter(grad_sums[1], ("twin", "dp"), scatter_dimension=0, tiled=True),
        lax.psum_scatter(grad_sums[2], ("twin", "dp"), scatter_dimension=0, tiled=True),
        lax.psum_scatter(grad_sums[3], ("twin", "dp"), scatter_dimension=0, tiled=True),
        lax.psum_scatter(grad_sums[4], ("twin", "dp"), scatter_dimension=0, tiled=True),
        lax.psum_scatter(grad_sums[5], ("twin", "dp"), scatter_dimension=0, tiled=True),
        lax.psum_scatter(grad_sums[6], ("twin", "dp"), scatter_dimension=0, tiled=True),
        lax.psum_scatter(grad_sums[7], ("twin", "dp"), scatter_dimension=0, tiled=True),
        lax.psum_scatter(grad_sums[8], ("twin", "dp"), scatter_dimension=0, tiled=True),
        lax.psum_scatter(grad_sums[9], ("twin", "dp"), scatter_dimension=0, tiled=True),
        lax.psum_scatter(grad_sums[10], ("twin", "dp"), scatter_dimension=0, tiled=True),
        lax.psum_scatter(grad_sums[11], ("twin", "dp"), scatter_dimension=0, tiled=True),
        lax.psum_scatter(grad_sums[12], ("twin", "dp"), scatter_dimension=0, tiled=True),
        lax.psum_scatter(grad_sums[13], ("twin", "dp"), scatter_dimension=0, tiled=True),
        lax.psum_scatter(grad_sums[14], ("twin", "dp"), scatter_dimension=0, tiled=True),
    )


def masked_scores(query_heads, key_heads, live_mask):
    raw_scores = jnp.einsum(
        "sqhd,skhd->shqk", query_heads, key_heads, preferred_element_type=jnp.float32
    ) * HDIM ** (-0.5)
    return jnp.where(live_mask[:, None, None, :], raw_scores, -1000000000.0)


def forward(tokens, live_mask, pool_weight, params):
    seq_count, seq_len, width = tokens.shape
    flat = tokens.reshape(seq_count * seq_len, width)
    head_shape = (seq_count, seq_len, HEADS, HDIM)
    query_heads = (product(flat, params[0]) + params[6]).astype(jnp.bfloat16).reshape(head_shape)
    key_heads = product(flat, params[1]).astype(jnp.bfloat16).reshape(head_shape)
    value_heads = (product(flat, params[2]) + params[7]).astype(jnp.bfloat16).reshape(head_shape)
    scores = masked_scores(query_heads, key_heads, live_mask)
    row_top = jnp.max(scores, axis=-1, keepdims=True)
    exp_terms = jnp.exp(scores - row_top)
    row_total = jnp.sum(exp_terms, axis=-1, keepdims=True)
    log_total = row_top + jnp.log(row_total)
    probs_low = (exp_terms / row_total).astype(jnp.bfloat16)
    mixed = jnp.einsum(
        "shqk,skhd->sqhd", probs_low, value_heads, preferred_element_type=jnp.float32
    )
    mixed = mixed.astype(jnp.bfloat16).reshape(seq_count * seq_len, width)
    first = flat.astype(jnp.float32) + (product(mixed, params[3]) + params[8])
    normed = layer_norm(first, params[9], params[10])
    inner = product(normed.astype(jnp.bfloat16), params[4]) + params[11]
    active = exact_gelu(inner).astype(jnp.bfloat16)
    second = normed + (product(active, params[5]) + params[12])
    output = layer_norm(second, params[13], params[14])
    pooled = jnp.sum(
        output.reshape(seq_count, seq_len, width) * pool_weight[:, :, None], axis=1
    ).astype(jnp.bfloat16)
    saved = (
        query_heads,
        key_heads,
        value_heads,
        log_total,
        mixed,
        first,
        normed,
        inner,
        active,
        second,
    )
    return (pooled, saved)


def backward(tokens, live_mask, pool_weight, params, saved, pool_grad):
    query_heads, key_heads, value_heads, log_total, mixed, first, normed, inner, active, second = (
        saved
    )
    seq_count, seq_len, width = tokens.shape
    flat = tokens.reshape(seq_count * seq_len, width)
    head_shape = (seq_count, seq_len, HEADS, HDIM)
    out_grad = (pool_weight[:, :, None] * pool_grad[:, None, :]).reshape(seq_count * seq_len, width)
    unused, second_pull = jax.vjp(
        layer_norm, second, params[13].astype(jnp.float32), params[14].astype(jnp.float32)
    )
    dsecond, dgain_two, dshift_two = second_pull(out_grad)
    dffn = dsecond.astype(jnp.bfloat16)
    dshrink_bias = column_sum(dffn)
    dshrink = product_lt(active, dffn)
    dactive = product_rt(dffn, params[5])
    unused, gelu_pull = jax.vjp(exact_gelu, inner)
    dinner = gelu_pull(dactive)[0].astype(jnp.bfloat16)
    dexpand_bias = column_sum(dinner)
    dexpand = product_lt(normed.astype(jnp.bfloat16), dinner)
    dnormed = dsecond + product_rt(dinner, params[4])
    unused, first_pull = jax.vjp(
        layer_norm, first, params[9].astype(jnp.float32), params[10].astype(jnp.float32)
    )
    dfirst, dgain_one, dshift_one = first_pull(dnormed)
    dbranch = dfirst.astype(jnp.bfloat16)
    dmixer_bias = column_sum(dbranch)
    dmixer = product_lt(mixed, dbranch)
    dmixed = product_rt(dbranch, params[3]).astype(jnp.bfloat16).reshape(head_shape)
    scores = masked_scores(query_heads, key_heads, live_mask)
    probs_full = jnp.exp(scores - log_total)
    probs_low = probs_full.astype(jnp.bfloat16)
    dvalue = jnp.einsum(
        "shqk,sqhd->skhd", probs_low, dmixed, preferred_element_type=jnp.float32
    ).astype(jnp.bfloat16)
    dprobs = jnp.einsum("sqhd,skhd->shqk", dmixed, value_heads, preferred_element_type=jnp.float32)
    row_delta = jnp.sum(probs_full * dprobs, axis=-1, keepdims=True)
    dscores = (probs_full * (dprobs - row_delta)).astype(jnp.bfloat16)
    dquery = (
        jnp.einsum("shqk,skhd->sqhd", dscores, key_heads, preferred_element_type=jnp.float32)
        * HDIM ** (-0.5)
    ).astype(jnp.bfloat16)
    dkey = (
        jnp.einsum("shqk,sqhd->skhd", dscores, query_heads, preferred_element_type=jnp.float32)
        * HDIM ** (-0.5)
    ).astype(jnp.bfloat16)
    dquery = dquery.reshape(seq_count * seq_len, width)
    dkey = dkey.reshape(seq_count * seq_len, width)
    dvalue = dvalue.reshape(seq_count * seq_len, width)
    dtokens = (
        dfirst
        + product_rt(dquery, params[0])
        + product_rt(dkey, params[1])
        + product_rt(dvalue, params[2])
    )
    grad_terms = (
        product_lt(flat, dquery),
        product_lt(flat, dkey),
        product_lt(flat, dvalue),
        dmixer,
        dexpand,
        dshrink,
        column_sum(dquery),
        column_sum(dvalue),
        dmixer_bias,
        dgain_one,
        dshift_one,
        dexpand_bias,
        dshrink_bias,
        dgain_two,
        dshift_two,
    )
    return (dtokens.reshape(seq_count, seq_len, width), grad_terms)


def staged_device(
    hidden_in,
    seq_lengths,
    pos_index,
    pos_count,
    query_proj,
    key_proj,
    value_proj,
    mixer_proj,
    expand_proj,
    shrink_proj,
    query_bias,
    value_bias,
    mixer_bias,
    first_gain,
    first_shift,
    expand_bias,
    shrink_bias,
    second_gain,
    second_shift,
):
    masters = (
        query_proj,
        key_proj,
        value_proj,
        mixer_proj,
        expand_proj,
        shrink_proj,
        query_bias,
        value_bias,
        mixer_bias,
        first_gain,
        first_shift,
        expand_bias,
        shrink_bias,
        second_gain,
        second_shift,
    )
    tower = lax.axis_index("twin")
    rank = lax.axis_index("dp")
    tokens_all = hidden_in[0]
    lengths_all = seq_lengths[0]
    per_micro = tokens_all.shape[0] // MICRO
    anchors = per_micro * lax.axis_size("dp")
    seq_len = tokens_all.shape[1]
    positions = jnp.arange(seq_len, dtype=jnp.int32)
    own_start = tower * anchors + rank * per_micro
    grad_total = None
    loss_total = jnp.zeros((), jnp.float32)
    input_grads = []
    for micro_step in range(MICRO):
        params = fetch_weights(masters)
        tokens = tokens_all[micro_step * per_micro : (micro_step + 1) * per_micro]
        lengths = lengths_all[micro_step * per_micro : (micro_step + 1) * per_micro]
        live_mask = positions[None, :] < lengths[:, None]
        pool_weight = live_mask.astype(jnp.float32) / lengths[:, None].astype(jnp.float32)
        pooled, saved = forward(tokens, live_mask, pool_weight, params)
        gathered = lax.all_gather(pooled, ("twin", "dp"), axis=0, tiled=True).astype(jnp.float32)
        pos_list = pos_index[micro_step]
        pos_num = pos_count[micro_step]
        loss_part, loss_pull = jax.vjp(
            lambda values: batch_loss(values, pos_list, pos_num), gathered
        )
        gathered_grad = loss_pull(jnp.ones((), jnp.float32))[0] * static_scale
        pool_grad = lax.dynamic_slice_in_dim(gathered_grad, own_start, per_micro, 0)
        dtokens, grad_terms = backward(tokens, live_mask, pool_weight, params, saved, pool_grad)
        input_grads.append(dtokens)
        loss_total = loss_total + loss_part
        grad_total = (
            grad_terms
            if grad_total is None
            else tuple((left + right for left, right in zip(grad_total, grad_terms)))
        )
    shards = settle_grads(grad_total)
    hidden_grad = jnp.concatenate(input_grads, axis=0)[None]
    loss_value = loss_total / (MICRO * anchors)
    return (
        loss_value,
        hidden_grad,
        shards[0],
        shards[1],
        shards[2],
        shards[3],
        shards[4],
        shards[5],
        shards[6],
        shards[7],
        shards[8],
        shards[9],
        shards[10],
        shards[11],
        shards[12],
        shards[13],
        shards[14],
    )


BF = jnp.bfloat16
F32 = jnp.float32
MESH = pl.DeviceIdType.MESH
VMEM_ALL = 67043328
TOK, WIDTH, INNER, SENT = 1024, 768, 3072, 512
SLOTS = 7
QB, VB, MB, G1, S1, EB, SB, G2, S2 = range(9)
VECTOR_SIZES = (24, 24, 24, 24, 24, 96, 24, 24, 24)
PIECES = (
    [(3, 16, 0, 128)]
    + [(0, 24, 0, 384), (0, 24, 384, 384)]
    + [(0, 24, 768 * j, 768) for j in range(1, 4)]
    + [(1, 24, 768 * j, 768) for j in range(4)]
    + [(2, 96, 256 * j, 256) for j in range(3)]
)
GRADS = (
    [(96, 24 * j, 0, 768) for j in range(4)]
    + [(24, 768 * j, 0, 768) for j in range(4)]
    + [(24, 0, 0, 768), (24, 768, 0, 768), (24, 1536, 0, 768)]
    + [(24, 2304, 0, 384), (24, 2304, 384, 384)]
)
VEC = len(GRADS)

AHEAD = 5
FORWARD = {'attend0': {0: ('g2', 'k5', 'a10'), 1: ('f2',), 2: ('g3',), 3: ('k7', 'a12')},
 'attend1': {0: ('k8',), 1: ('g4',), 2: ('i6', 'k9', 'f4')},
 'attend2': {0: ('k10',), 1: ('g5',), 3: ('f5', 'i8', 'k11', 'g6')},
 'exp0': {0: ('k12',), 1: ('g7',), 4: ('f7',), 5: ('i10',)},
 'exp1': {1: ('g8',), 4: ('f8',), 5: ('i11',)},
 'exp2': {1: ('g9',), 4: ('f9',), 5: ('i12',)},
 'exp3': {2: ('g10',), 5: ('f10', 'g11')},
 'mix': {3: ('f6', 'i9')},
 'proj0': {-1: ('f1',), 1: ('i3',)},
 'proj1': {-1: ('f3',), 2: ('i5',)},
 'proj2': {4: ('i7',)},
 'projh': {0: ('i4',), 1: ('k6', 'a11')},
 'shr1': {-1: ('g12', 'f11')},
 'shr2': {-1: ('f12',)},
 'vec': {-1: ('k0',
              'a5',
              'k1',
              'a6',
              'i0',
              'k2',
              'a7',
              'i1',
              'g0',
              'k3',
              'a8',
              'i2',
              'f0'),
         5: ('g1',),
         7: ('k4', 'a9')}}
BACKWARD = {'actb': {2: ('c0', 'r0'),
          3: ('c1', 'r1'),
          4: ('c2', 'r2', 'c3', 'r3'),
          6: ('d0',),
          8: ('d1',),
          10: ('d2',)},
 'attb0': {0: ('c8', 's5', 'r8'), 2: ('f4', 's6'), 3: ('s7', 'f5')},
 'attb1': {1: ('f6', 's8', 'c9', 'r9'), 2: ('f7',), 3: ('d9',)},
 'attb2': {0: ('f8',), 1: ('s9', 'c10', 'r10'), 2: ('c11', 'r11'), 3: ('d10',)},
 'expg0': {0: ('d3',)},
 'expg1': {1: ('s0',)},
 'expg2': {0: ('c4', 'r4'), 2: ('s1', 'c5', 'r5')},
 'expg3': {2: ('s2',)},
 'firstb': {0: ('r6',),
            1: ('f1', 's3', 'd4', 'c7', 'r7'),
            2: ('f2', 'd5', 'd6')},
 'inb': {0: ('c12', 's10', 'r12', 'c13', 'r13'),
         1: ('s11',),
         2: ('d12', 'd13')},
 'ing0': {0: ('d8',)},
 'ingh1': {0: ('f9',), 1: ('d11',)},
 'mixb': {0: ('f3', 'd7')},
 'mixg': {1: ('s4',)},
 'st7': {-1: ('c6', 'f0')},
 'tail': {-1: ('f10', 's12', 's13', 'f11', 'f12', 'f13')}}


def coords():
    rank = lax.axis_index("dp")
    return lax.axis_index("twin"), rank // 4, (rank // 2) % 2, rank % 2


def flat(t, z, y, c):
    return t * 16 + z * 4 + y * 2 + c


def dev(t, z, y, c):
    return {"twin": t, "dp": z * 4 + y * 2 + c}


def neighbours(t, z, y, c):
    return [dev(t, (z + k) % 4, y, c) for k in (1, 2, 3)] + [
        dev(1 - t, z, y, c),
        dev(t, z, 1 - y, c),
        dev(t, z, y, 1 - c),
    ]


def signal_all(sem):
    for other in neighbours(*coords()):
        pl.semaphore_signal(sem, inc=1, device_id=other, device_id_type=MESH)


def send(src, dst, send_sem, recv_sem, target):
    pltpu.make_async_remote_copy(
        src, dst, send_sem, recv_sem, device_id=target, device_id_type=MESH
    ).start()


def wait_bytes(ref, sem):
    pltpu.make_async_copy(ref, ref, sem).wait()


class Gather:
    def __init__(self, arrays, recv, sent):
        self.arrays, self.recv, self.sent = arrays, recv, sent
        self.at = coords()

    def rows(self, p, owner):
        w, r, c0, nc = PIECES[p]
        return self.arrays[w].at[pl.ds(pl.multiple_of(owner * r, 8), r), pl.ds(c0, nc)]

    def halves(self, p, owners, half):
        w, r, c0, nc = PIECES[p]
        if nc % 256:
            return [self.rows(p, owner) for owner in owners[2 * half : 2 * half + 2]]
        cols = pl.ds(c0 + half * (nc // 2), nc // 2)
        return [
            self.arrays[w].at[pl.ds(pl.multiple_of(owner * r, 8), r), cols] for owner in owners
        ]

    def put(self, p, part, target, group):
        send(part, part, self.sent.at[p], self.recv.at[p, group], target)

    def wait(self, p, group, shards):
        w, r, c0, nc = PIECES[p]
        wait_bytes(
            self.arrays[w].at[pl.ds(0, shards * r), pl.ds(c0, nc)], self.recv.at[p, group]
        )

    def start(self, p):
        t, z, y, c = self.at
        own = self.rows(p, flat(t, z, y, c))
        for k in (1, 2, 3):
            self.put(p, own, dev(t, (z + k) % 4, y, c), 0)
        self.put(p, own, dev(1 - t, z, y, c), 1)
        self.put(p, own, dev(t, z, 1 - y, c), 2)
        self.put(p, own, dev(t, z, y, 1 - c), 5)

    def column(self, p):
        t, z, y, c = self.at
        self.wait(p, 0, 3)
        for k in (1, 2, 3):
            part = self.rows(p, flat(t, (z + k) % 4, y, c))
            self.put(p, part, dev(1 - t, z, y, c), 1)
            self.put(p, part, dev(t, z, 1 - y, c), 2)
            self.put(p, part, dev(t, z, y, 1 - c), 5)

    def sides(self, p):
        t, z, y, c = self.at
        self.wait(p, 1, 4)
        owners = [flat(1 - t, k, y, c) for k in range(4)]
        for part in self.halves(p, owners, 0):
            self.put(p, part, dev(t, z, 1 - y, c), 4)
        for owner in owners:
            self.put(p, self.rows(p, owner), dev(t, z, y, 1 - c), 5)
        self.wait(p, 2, 4)
        owners = [flat(t, k, 1 - y, c) for k in range(4)]
        for part in self.halves(p, owners, 1):
            self.put(p, part, dev(1 - t, z, y, c), 3)
        for owner in owners:
            self.put(p, self.rows(p, owner), dev(t, z, y, 1 - c), 5)

    def diagonal(self, p):
        t, z, y, c = self.at
        owners = [flat(1 - t, k, 1 - y, c) for k in range(4)]
        for group, half in ((3, 1), (4, 0)):
            self.wait(p, group, 2)
            for part in self.halves(p, owners, half):
                self.put(p, part, dev(t, z, y, 1 - c), 5)

    def finish(self, p):
        self.wait(p, 5, 16)

    def drain(self, p):
        w, r, c0, nc = PIECES[p]
        wait_bytes(self.arrays[w].at[pl.ds(0, 31 * r), pl.ds(c0, nc)], self.sent.at[p])

    def table(self):
        return {
            "a": self.start,
            "k": self.column,
            "i": self.sides,
            "g": self.diagonal,
            "f": self.finish,
        }


class Scatter:
    def __init__(self, grad, bufs, vec_grad, vec_bufs, recv, sent, free, store):
        self.grad, self.bufs, self.vec_grad, self.vec_bufs = grad, bufs, vec_grad, vec_bufs
        self.recv, self.sent, self.free, self.store = recv, sent, free, store
        self.at = coords()

    def size(self, p):
        return (16, 128) if p == VEC else (24, GRADS[p][3])

    def buf(self, p, which):
        if p == VEC:
            return self.vec_bufs[which]
        whole = self.bufs[which].at[p % SLOTS]
        if GRADS[p][3] == 768:
            return whole
        cols = pl.ds(0, 384)
        if which == 0:
            return whole.at[:, cols]
        if which == 1:
            return whole.at[:, pl.ds(0, 48), :]
        return whole.at[:, :, cols]

    def part(self, p, owner):
        if p == VEC:
            return self.vec_grad.at[pl.ds(pl.multiple_of(owner * 16, 8), 16), :]
        stride, base, col, cols = GRADS[p]
        return self.grad.at[
            pl.ds(pl.multiple_of(owner * stride + base, 8), 24), pl.ds(col, cols)
        ]

    def mine(self, p, t, z, y, n=1):
        r, nc = self.size(p)
        first = pl.multiple_of((t * 8 + y * 4 + z) * r, 8)
        return self.buf(p, 0).at[pl.ds(first, n * r), :]

    def half(self, p, t, y, half):
        r, nc = self.size(p)
        first = (t * 8 + y * 4) * r
        if nc < 768:
            first = pl.multiple_of(first + half * 2 * r, 8)
            return self.buf(p, 0).at[pl.ds(first, 2 * r), :]
        return self.buf(p, 0).at[
            pl.ds(pl.multiple_of(first, 8), 4 * r), pl.ds(half * (nc // 2), nc // 2)
        ]

    def put(self, p, group, src, dst, target, lane=1):
        send(src, dst, self.sent.at[p, lane], self.recv.at[p, group], target)

    def start(self, p):
        t, z, y, c = self.at
        if SLOTS <= p < VEC:
            pl.semaphore_wait(self.free.at[p % SLOTS], 6)

        def body(i, carry):
            tt, yy, zz = i // 8, (i // 4) % 2, i % 4
            src = self.part(p, flat(tt, zz, yy, 1 - c))
            self.put(p, 0, src, self.mine(p, tt, zz, yy), dev(t, z, y, 1 - c), 0)
            return carry

        lax.fori_loop(0, 16, body, 0)

    def add_columns(self, p, first, last):
        t, z, y, c = self.at

        def body(i, carry):
            tt = (t + 1 - i // 8) % 2
            yy = (y + 1 - (i // 4) % 2) % 2
            a = self.mine(p, tt, i % 4, yy)
            b = self.part(p, flat(tt, i % 4, yy, c))
            a[...] = a[...] + b[...]
            return carry

        lax.fori_loop(first, last, body, 0)

    def cores(self, p):
        t, z, y, c = self.at
        wait_bytes(self.buf(p, 0), self.recv.at[p, 0])
        self.add_columns(p, 0, 4)
        diag = self.buf(p, 1)
        self.put(p, 2, self.half(p, 1 - t, 1 - y, 0), diag.at[0], dev(t, z, 1 - y, c))
        self.put(p, 1, self.half(p, 1 - t, 1 - y, 1), diag.at[1], dev(1 - t, z, y, c))
        self.add_columns(p, 4, 16)

    def add(self, a, b):
        a[...] = a[...] + b[...]

    def diagonals(self, p):
        t, z, y, c = self.at
        diag, side = self.buf(p, 1), self.buf(p, 2)
        wait_bytes(diag.at[0], self.recv.at[p, 2])
        self.add(self.half(p, 1 - t, y, 0), diag.at[0])
        self.put(p, 3, self.mine(p, 1 - t, 0, y, 4), side.at[0], dev(1 - t, z, y, c))
        wait_bytes(diag.at[1], self.recv.at[p, 1])
        self.add(self.half(p, t, 1 - y, 1), diag.at[1])
        self.put(p, 4, self.mine(p, t, 0, 1 - y, 4), side.at[1], dev(t, z, 1 - y, c))

    def sides(self, p):
        t, z, y, c = self.at
        side, col = self.buf(p, 2), self.buf(p, 3)
        wait_bytes(side.at[0], self.recv.at[p, 3])
        wait_bytes(side.at[1], self.recv.at[p, 4])
        a = self.mine(p, t, 0, y, 4)
        total = a[...].astype(F32) + side[0].astype(F32) + side[1].astype(F32)
        a[...] = total.astype(a.dtype)
        for k in (1, 2, 3):
            zz = (z + k) % 4
            self.put(p, 5, self.mine(p, t, zz, y), col.at[k - 1], dev(t, zz, y, c))

    def finish(self, p):
        t, z, y, c = self.at
        col = self.buf(p, 3)
        wait_bytes(col, self.recv.at[p, 5])
        total = self.mine(p, t, z, y)[...].astype(F32)
        for k in range(3):
            total = total + col[k].astype(F32)
        self.store(p, total)
        self.drain(p)
        if p + SLOTS < VEC:
            signal_all(self.free.at[p])

    def drain(self, p):
        r, nc = self.size(p)
        wait_bytes(self.buf(p, 0).at[pl.ds(0, 15 * r), :], self.sent.at[p, 1])

    def table(self):
        return {
            "c": self.cores,
            "d": self.diagonals,
            "s": self.sides,
            "f": self.finish,
            "r": self.release,
        }

    def release(self, p):
        wait_bytes(self.buf(p, 0), self.sent.at[p, 0])


def dot(a, b):
    return jnp.dot(a, b, preferred_element_type=F32)


def dot_lt(a, b):
    return lax.dot_general(a, b, (((0,), (0,)), ((), ())), preferred_element_type=F32)


def dot_rt(a, b):
    return lax.dot_general(a, b, (((1,), (1,)), ((), ())), preferred_element_type=F32)


def block(i, n):
    return pl.ds(pl.multiple_of(i * n, n), n)


def iota(shape, axis):
    return lax.broadcasted_iota(jnp.int32, shape, axis)


def loop(n, body, ticks=()):
    ticks = {k: v for k, v in dict(ticks).items() if k >= 0}

    def step(i, carry):
        body(i)
        for k, tick in ticks.items():

            @pl.when(i == k)
            def _(tick=tick):
                for part in tick:
                    part()

        return carry

    lax.fori_loop(0, n, step, 0)


def ticks_of(plan, name, table):
    return {
        k: [lambda n=n: table[n[0]](int(n[1:])) for n in names]
        for k, names in plan.get(name, {}).items()
    }


def owner_of(n, size):
    owner = jnp.floor((n.astype(F32) + 0.5) * (1.0 / size)).astype(jnp.int32)
    return owner, n - owner * size


def vector_row(vec, k):
    size = VECTOR_SIZES[k]
    width = 32 * size
    owner, place = owner_of(iota((1, width), 1), size)
    shards = vec[pl.ds(k, 32, stride=16), :].astype(BF)
    pick = jnp.where(iota((128, width), 0) == place, 1.0, 0.0).astype(BF)
    spreaded = dot(shards, pick)
    return jnp.sum(jnp.where(iota((32, width), 0) == owner, spreaded, 0.0), axis=0, keepdims=True)


def vector_tiles(row, k):
    size = VECTOR_SIZES[k]
    width = 32 * size
    owner, place = owner_of(iota((1, width), 1), size)
    pick = jnp.where(iota((128, width), 0) == place, 1.0, 0.0)
    parts = jnp.where(iota((32, width), 0) == owner, row, 0.0)
    return lax.dot_general(
        parts,
        pick,
        (((1,), (1,)), ((), ())),
        precision=lax.Precision.HIGHEST,
        preferred_element_type=F32,
    )


def normalize(v):
    center = v - jnp.mean(v, axis=1, keepdims=True)
    spread_ = jnp.mean(center * center, axis=1, keepdims=True)
    scale = lax.rsqrt(spread_ + norm_eps)
    return center * scale, scale


def contrast(pool, pos, cnt, dpool, own):
    total = jnp.zeros((1, 1), F32)
    row, col = iota((32, 32), 0), iota((32, 32), 1)
    valid = (row < 16) & (col >= 16)
    eye = row == col
    for m in range(MICRO):
        chunks = [pool[pl.ds(8 * m + k, 32, stride=16), :] for k in range(6)]
        gram = jnp.zeros((32, 32), F32)
        for chunk in chunks:
            gram = gram + dot_rt(chunk.astype(BF), chunk.astype(BF))
        diag = jnp.where(eye, gram, 0.0)
        scale_c = lax.rsqrt(jnp.sum(diag, axis=1, keepdims=True) + 1e-6)
        scale_r = lax.rsqrt(jnp.sum(diag, axis=0, keepdims=True) + 1e-6)
        sims = cosine_scale * gram * scale_c * scale_r
        top = jnp.max(jnp.where(valid, sims, -1e30), axis=1, keepdims=True)
        terms = jnp.where(valid, jnp.exp(jnp.minimum(sims - top, 0.0)), 0.0)
        row_sum = jnp.where(row[:, :1] < 16, jnp.sum(terms, axis=1, keepdims=True), 1.0)
        logs = jnp.where(row[:, :1] < 16, top + jnp.log(row_sum), 0.0)
        hits = jnp.zeros((16, 32), F32)
        eye16 = iota((16, 16), 0) == iota((16, 16), 1)
        number = jnp.sum(jnp.where(eye16, cnt[m : m + 1, :], 0), axis=1, keepdims=True)
        for k in range(6):
            hit = (pos[m, :, k : k + 1] + 16 == iota((16, 32), 1)) & (k < number)
            hits = hits + jnp.where(hit, 1.0, 0.0)
        target = jnp.concatenate([hits / number.astype(F32), jnp.zeros((16, 32), F32)], axis=0)
        loss = logs - jnp.sum(target * sims, axis=1, keepdims=True)
        total = total + jnp.sum(jnp.where(row[:, :1] < 16, loss, 0.0), axis=0, keepdims=True)
        grad = (terms / row_sum - target) * static_scale
        mine_r = jnp.sum(jnp.where(row == own, grad * scale_r, 0.0), axis=0, keepdims=True)
        weight = jnp.sum(jnp.where(eye, mine_r, 0.0), axis=1, keepdims=True)
        weight = weight + jnp.sum(
            jnp.where(col == own, grad * scale_c, 0.0), axis=1, keepdims=True
        )
        weight = cosine_scale * weight
        mine = iota((32, 1), 0) == own
        scale = jnp.sum(jnp.where(mine, scale_c, 0.0), axis=0, keepdims=True)
        along = jnp.zeros((1, 1), F32)
        pulls = []
        for chunk in chunks:
            pull = jnp.sum(weight * chunk, axis=0, keepdims=True)
            x = jnp.sum(jnp.where(mine, chunk, 0.0), axis=0, keepdims=True)
            along = along + jnp.sum(pull * x, axis=1, keepdims=True)
            pulls.append((pull, x))
        for k, (pull, x) in enumerate(pulls):
            dpool[m : m + 1, 128 * k : 128 * k + 128] = scale * pull - x * (
                scale * scale * scale * along
            )
    return total


def step_kernel(*refs):
    (lens, tokens, pos, cnt, mq, mk, mv, mm, me, ms) = refs[:10]
    mvec = refs[10:19]
    (loss, hidden, probs, gq, gk, gv, gm, ge, gs, gvec) = refs[19:29]
    (wa, we, ws, vec, grad, rc, rd, rs, rz, act, gp, qkv, mixed, nb, n1, n2) = refs[29:45]
    (f1, pbuf, r1, r2, par, pgrad, nbar, dpool, pool, poolf) = refs[45:55]
    (vc, vd, vs, vz) = refs[55:59]
    vgrad = vec
    (g_recv, g_sent, s_recv, s_sent, free, pool_recv, pool_sent, p_sem, h_sem, in_sem, x) = refs[59:]
    t, z, y, c = coords()
    own = flat(t, z, y, c)
    gather = Gather((wa, we, ws, vec), g_recv, g_sent)

    rows = (0, 24, 48, 72, 192, 216, 240, 264, 96)
    wide = [me.at[:, pl.ds(768 * j, 768)] for j in range(4)]
    loads = [
        pltpu.make_async_copy(shard, f1.at[pl.ds(row, shard.shape[0]), :], in_sem.at[k])
        for k, (row, shard) in enumerate(zip(rows, [mq, mk, mv, mm, *wide, ms]))
    ]
    loads.append(pltpu.make_async_copy(tokens, x, in_sem.at[9]))
    for load in loads:
        load.start()
    barrier = pltpu.get_barrier_semaphore()
    signal_all(barrier)
    here24 = pl.ds(pl.multiple_of(own * 24, 8), 24)
    here16 = pl.ds(pl.multiple_of(own * 16, 8), 16)
    vec[here16, :] = jnp.zeros((16, 128), F32)
    for k, size in enumerate(VECTOR_SIZES):
        vec[pl.ds(own * 16 + k, 1), 0:size] = (
            mvec[k][...].reshape(1, size).astype(BF).astype(F32)
        )
    pl.semaphore_wait(barrier, 6)
    gather.start(0)
    for load in loads[:3]:
        load.wait()
    for g in range(6):
        for j in range(3):
            first = 384 * g + 128 * j
            shard = f1[24 * j : 24 * j + 24, 128 * g : 128 * g + 128]
            wa[here24, first : first + 128] = shard.astype(BF)
        if g in (0, 1, 3, 5):
            gather.start((g + 3) // 2 if g else 1)
    for load in loads[3:9]:
        load.wait()
    wa[here24, 2304:3072] = f1[72:96, :].astype(BF)
    for j in range(4):
        we[here24, 768 * j : 768 * j + 768] = f1[192 + 24 * j : 216 + 24 * j, :].astype(BF)
    ws[pl.ds(pl.multiple_of(own * 96, 8), 96), :] = f1[96:192, :].astype(BF)

    def planned(name):
        ticks = ticks_of(FORWARD, name, gather.table())
        for part in ticks.get(-1, ()):
            part()
        return ticks

    ticks = planned("vec")
    for k, size in enumerate(VECTOR_SIZES):
        par[k : k + 1, 0 : 32 * size] = vector_row(vec, k)
        for part in ticks.get(k, ()):
            part()

    for g in range(6):
        lanes, first = slice(128 * g, 128 * g + 128), 384 * g
        par[9:10, first : first + 128] = par[QB : QB + 1, lanes] * HDIM ** (-0.5)
        par[9:10, first + 128 : first + 256] = jnp.zeros((1, 128), F32)
        par[9:10, first + 256 : first + 384] = par[VB : VB + 1, lanes]
        par[10:11, first : first + 128] = jnp.full((1, 128), HDIM ** (-0.5), F32)
        par[10:11, first + 128 : first + 384] = jnp.ones((1, 256), F32)
    loads[9].wait()

    first_head = iota((SENT, 128), 1) < 64

    def put_probs(slot, item):
        return pltpu.make_async_copy(pbuf.at[slot], probs.at[item], p_sem.at[slot])

    def project(first, size, blocks):
        def body(i):
            rows = block(i // blocks, 512)
            cols = pl.ds(pl.multiple_of(first + i % blocks * size, 128), size)
            value = dot(x[rows, :], wa[:, cols])
            qkv[rows, cols] = (value * par[10:11, cols] + par[9:10, cols]).astype(BF)

        return body

    def second_half():
        loop(2, project(384, 384, 1), planned("projh"))

    def triple(pair):
        return [pl.ds(pl.multiple_of(384 * pair + 128 * n, 128), 128) for n in range(3)]

    def attend(g):
        def body(i):
            item = 4 * g + i
            s, j = i % 2, i // 2
            slot = item % 2
            rows = block(s, SENT)
            live = iota((1, SENT), 1) < lens[s]
            if g:
                put_probs(slot, item - 2).wait()
            else:

                @pl.when(i >= 2)
                def _():
                    put_probs(slot, item - 2).wait()

            q, k, v = [qkv[rows, cols] for cols in triple(2 * g + j)]
            zero = jnp.zeros_like(q)
            outs = []
            for h in range(2):
                qh = jnp.where(first_head if h == 0 else ~first_head, q, zero)
                scores = jnp.where(live, dot_rt(qh, k), -1000000000.0)
                terms = jnp.exp(scores - jnp.max(scores, axis=1, keepdims=True))
                low = (terms * (1.0 / jnp.sum(terms, axis=1, keepdims=True))).astype(BF)
                pbuf[slot, h] = low
                outs.append(dot(low, v))
            mixed[rows, block(2 * g + j, 128)] = jnp.where(first_head, outs[0], outs[1]).astype(BF)
            put_probs(slot, item).start()

        return body

    for g in range(3):
        if g == 0:
            loop(2, project(0, 384, 1), planned("proj0"))
        else:
            loop(6, project(768 * g, 256, 3), planned("proj%d" % g))
        ticks = planned("attend%d" % g)
        if g == 0:
            ticks.setdefault(1, []).append(second_half)
        loop(4, attend(g), ticks)
    for item in (10, 11):
        put_probs(item % 2, item).wait()

    def mix(i):
        rows = block(i, 256)
        first = dot(mixed[rows, :], wa[:, 2304:3072]) + par[MB : MB + 1, 0:768]
        n, r = normalize(x[rows, :].astype(F32) + first)
        n1[rows, :] = n.astype(BF)
        r1[rows, :] = r
        normed = n * par[G1 : G1 + 1, 0:768] + par[S1 : S1 + 1, 0:768]
        f1[rows, :] = normed
        nb[rows, :] = normed.astype(BF)

    loop(4, mix, planned("mix"))

    for j in range(4):

        def expand(i, j=j):
            rows, cols = block(i % 2, 512), block(3 * j + i // 2, 256)
            v = dot(nb[rows, :], we[:, cols]) + par[EB : EB + 1, cols]
            phi = 0.5 + 0.5 * lax.erf(v * 0.7071067811865476)
            act[rows, cols] = (v * phi).astype(BF)
            slope = phi + v * (jnp.exp(-0.5 * (v * v)) * 0.3989422804014327)
            gp[rows, cols] = slope.astype(BF)

        loop(6, expand, planned("exp%d" % j))
    for j in range(3):

        def shrink(i, j=j):
            rows, cols = block(i, 512), slice(256 * j, 256 * j + 256)
            value = dot(act[rows, :], ws[:, cols]) + par[SB : SB + 1, cols]
            f1[rows, cols] = f1[rows, cols] + value

        loop(2, shrink, planned("shr%d" % j))

    nbar[...] = jnp.zeros_like(nbar)

    def weight_of(i, n):
        s = (i * n) // SENT
        length = lens[s]
        token = iota((n, 1), 0) + (i * n - s * SENT)
        return jnp.where(token < length, 1.0, 0.0) / length.astype(F32)

    def finish_norm(i):
        rows = block(i, 128)
        n, r = normalize(f1[rows, :])
        w = weight_of(i, 128)
        n2[rows, :] = n.astype(BF)
        r2[rows, :] = r * w
        total = jnp.sum(n * w, axis=0, keepdims=True)
        s = i // 4
        nbar[pl.ds(s, 1), :] = nbar[pl.ds(s, 1), :] + total

    loop(8, finish_norm)
    pooled = nbar[0:2, :] * par[G2 : G2 + 1, 0:768] + par[S2 : S2 + 1, 0:768]
    tile = jnp.zeros((16, 128), F32)
    place = iota((16, 128), 0)
    for m in range(2):
        for k in range(6):
            tile = jnp.where(place == 8 * m + k, pooled[m : m + 1, 128 * k : 128 * k + 128], tile)
    at = pool.at[pl.ds(pl.multiple_of(own * 16, 8), 16), :]
    at[...] = tile.astype(BF)

    def spread_pool(i, carry):
        other = lax.rem(own + i, 32)
        target = {"twin": other // 16, "dp": lax.rem(other, 16)}
        send(at, at, pool_sent, pool_recv, target)
        return carry

    lax.fori_loop(1, 32, spread_pool, 0)
    for p in range(len(PIECES)):
        gather.drain(p)
    wait_bytes(pool.at[pl.ds(0, 496), :], pool_recv)
    poolf[...] = pool[...].astype(F32)
    loss[...] = contrast(poolf, pos, cnt, dpool, own) / (MICRO * 16)
    wait_bytes(pool.at[pl.ds(0, 496), :], pool_sent)

    def store(p, total):
        if p == VEC:
            gvec[...] = total
        elif p < 4:
            gs[24 * p : 24 * p + 24, :] = total
        elif p < 8:
            ge[:, 768 * (p - 4) : 768 * (p - 4) + 768] = total
        elif p == 8:
            gm[...] = total
        else:
            for j in range(total.shape[1] // 384):
                pair = 2 * (p - 9) + j if p < 11 else p - 7
                for n, ref in enumerate((gq, gk, gv)):
                    first = 384 * j + 128 * n
                    ref[:, 128 * pair : 128 * pair + 128] = total[:, first : first + 128]

    scatter = Scatter(
        grad, (rc, rd, rs, rz), vgrad, (vc, vd, vs, vz), s_recv, s_sent, free, store
    )
    pgrad[...] = jnp.zeros_like(pgrad)
    gain2 = par[G2 : G2 + 1, 0:768]
    pgrad[G2 : G2 + 1, 0:768] = jnp.sum(dpool[0:2, :] * nbar[0:2, :], axis=0, keepdims=True)
    pgrad[S2 : S2 + 1, 0:768] = jnp.sum(dpool[0:2, :], axis=0, keepdims=True)

    def collect(k, value):
        cols = slice(0, 32 * VECTOR_SIZES[k])
        pgrad[k : k + 1, cols] = pgrad[k : k + 1, cols] + jnp.sum(value, axis=0, keepdims=True)

    def second_back(i):
        rows = block(i, 128)
        u = dpool[pl.ds(i // 4, 1), :] * gain2
        u = u - jnp.mean(u, axis=1, keepdims=True)
        n = n2[rows, :].astype(F32)
        along = jnp.mean(n * u, axis=1, keepdims=True)
        back = r2[rows, :] * (u - n * along)
        f1[rows, :] = back
        low = back.astype(BF)
        n2[rows, :] = low
        collect(SB, low.astype(F32))

    loop(8, second_back)

    def shrink_grad(i):
        grad[block(i, 256), :] = dot_lt(act[:, block(i, 256)], n2[...]).astype(BF)

    loop(12, shrink_grad)
    for p in range(4):
        scatter.start(p)

    def planned(name):
        ticks = ticks_of(BACKWARD, name, scatter.table())
        for part in ticks.get(-1, ()):
            part()
        return ticks

    def act_back(i):
        cols = block(i, 256)
        back = dot_rt(n2[...], ws[cols, :]) * gp[:, cols].astype(F32)
        low = back.astype(BF)
        gp[:, cols] = low
        pgrad[EB : EB + 1, cols] = jnp.sum(low.astype(F32), axis=0, keepdims=True)

    loop(12, act_back, planned("actb"))
    planned("expg")

    def expand_grad(i, j):
        cols = block(3 * j + i, 256)
        grad[768 * j : 768 * j + 768, block(i, 256)] = dot_lt(nb[...], gp[:, cols]).astype(BF)

    for j in range(4):
        loop(3, lambda i, j=j: expand_grad(i, j), planned("expg%d" % j))
        planned("st%d" % (4 + j))
        scatter.start(4 + j)

    def first_back(i):
        rows = block(i, 256)
        back = f1[rows, :] + dot_rt(gp[rows, :], we[...])
        n = n1[rows, :].astype(F32)
        collect(G1, back * n)
        collect(S1, back)
        dn = back * par[G1 : G1 + 1, 0:768]
        mean = jnp.mean(dn, axis=1, keepdims=True)
        along = jnp.mean(dn * n, axis=1, keepdims=True)
        back = r1[rows, :] * (dn - mean - n * along)
        f1[rows, :] = back
        low = back.astype(BF)
        n2[rows, :] = low
        collect(MB, low.astype(F32))

    loop(4, first_back, planned("firstb"))

    def mixer_grad(i):
        grad[0:768, block(i, 256)] = dot_lt(mixed[...], n2[:, block(i, 256)]).astype(BF)

    loop(3, mixer_grad, planned("mixg"))
    planned("st8")
    scatter.start(8)

    def get_probs(item):
        return pltpu.make_async_copy(probs.at[item], pbuf.at[item % 2], p_sem.at[item % 2])

    get_probs(0).start()
    get_probs(1).start()

    def mixed_back(i):
        rows = block(i, 512)
        n2[rows, :] = dot_rt(n2[rows, :], wa[:, 2304:3072]).astype(BF)

    loop(2, mixed_back, planned("mixb"))
    planned("att")

    for g in range(3):

        def attend_back(i, g=g):
            s, j = i % 2, i // 2
            pair = 2 * g + j
            item = 4 * g + i
            slot = i % 2
            rows = block(s, SENT)
            get_probs(item).wait()
            q, k, v = [qkv[rows, cols] for cols in triple(pair)]
            do = n2[rows, block(pair, 128)]
            zero = jnp.zeros_like(do)
            both = do.astype(F32) * mixed[rows, block(pair, 128)].astype(F32)
            parts = []
            for h in range(2):
                head = first_head if h == 0 else ~first_head
                p = pbuf[slot, h]
                delta = jnp.sum(jnp.where(head, both, 0.0), axis=1, keepdims=True)
                dp = dot_rt(jnp.where(head, do, zero), v)
                ds = (p.astype(F32) * (dp - delta)).astype(BF)
                parts.append((dot(ds, k) * (HDIM ** (-0.5)), dot_lt(ds, q), dot_lt(p, do)))
            for n, cols in enumerate(triple(pair)):
                value = jnp.where(first_head, parts[0][n], parts[1][n])
                act[rows, cols] = value.astype(BF)

            @pl.when(item + 2 < 12)
            def _():
                get_probs(item + 2).start()

        def half_grad(j):
            def body(i):
                cols = pl.ds(1536 + 384 * j, 384)
                grad[pl.ds(pl.multiple_of(2304 + 384 * i, 8), 384), 384 * j : 384 * j + 384] = (
                    dot_lt(x[:, block(i, 384)], act[:, cols]).astype(BF)
                )

            loop(2, body, planned("ingh%d" % j))
            planned("st%d" % (11 + j))
            scatter.start(11 + j)

        def input_grad(i, g=g):
            grad[768 * (g + 1) : 768 * (g + 2), block(i, 256)] = dot_lt(
                x[...], act[:, block(3 * g + i, 256)]
            ).astype(BF)

        ticks = planned("attb%d" % g)
        if g == 2:
            ticks.setdefault(1, []).append(lambda: half_grad(0))
        loop(4, attend_back, ticks)
        if g == 2:
            half_grad(1)
        else:
            loop(3, input_grad, planned("ing%d" % g))
            planned("st%d" % (9 + g))
            scatter.start(9 + g)
        for j in range(2):
            first, lanes = 768 * g + 384 * j, slice(256 * g + 128 * j, 256 * g + 128 * j + 128)
            for k, col in ((QB, first), (VB, first + 256)):
                pgrad[k : k + 1, lanes] = jnp.sum(
                    act[:, col : col + 128].astype(F32), axis=0, keepdims=True
                )
    for k in range(9):
        tiles = vector_tiles(pgrad[k : k + 1, 0 : 32 * VECTOR_SIZES[k]], k)
        vgrad[pl.ds(k, 32, stride=16), :] = tiles
    scatter.start(VEC)

    def put_hidden(i):
        rows = block(i, 256)
        return pltpu.make_async_copy(f1.at[rows, :], hidden.at[rows, :], h_sem.at[i])

    def input_back(i):
        rows = block(i, 256)
        f1[rows, :] = f1[rows, :] + dot_rt(act[rows, 0:2304], wa[:, 0:2304])
        put_hidden(i).start()

    loop(4, input_back, planned("inb"))
    planned("tail")
    for i in range(4):
        put_hidden(i).wait()


def emit_kernel(*refs):
    hidden, shards, gvec, loss = refs[0], refs[1:7], refs[7], refs[8]
    hidden_o, shards_o, vectors_o, loss_o = refs[9], refs[10:16], refs[16:25], refs[25]
    held, parts, sem_in, sem_out = refs[26], refs[27:33], refs[33], refs[34]
    moves = [
        (hidden.at[block(k, 128), :], held.at[block(k, 128), :], hidden_o.at[block(k, 128), :])
        for k in range(8)
    ] + list(zip(shards, parts, shards_o))
    for k, (src, mid, _) in enumerate(moves):
        pltpu.make_async_copy(src, mid, sem_in.at[k]).start()
    for k, size in enumerate(VECTOR_SIZES):
        vectors_o[k][...] = gvec[k, 0:size]
    loss_o[0] = loss[0, 0]
    for k, (src, mid, dst) in enumerate(moves):
        pltpu.make_async_copy(src, mid, sem_in.at[k]).wait()
        pltpu.make_async_copy(mid, dst, sem_out.at[k]).start()
    for k, (_, mid, dst) in enumerate(moves):
        pltpu.make_async_copy(mid, dst, sem_out.at[k]).wait()


def fused_device(hidden_in, seq_lengths, pos_index, pos_count, *masters):
    x = hidden_in.reshape(TOK, WIDTH)
    whole = pl.BlockSpec(memory_space=pltpu.VMEM)
    scalars = pl.BlockSpec(memory_space=pltpu.SMEM)
    away = pl.BlockSpec(memory_space=pl.ANY)
    shape = jax.ShapeDtypeStruct
    square = shape((24, 768), F32)
    shards = [square] * 4 + [shape((24, 3072), F32), shape((96, 768), F32)]
    pieces = len(PIECES)
    outs = pl.pallas_call(
        step_kernel,
        out_shape=[
            shape((1, 1), F32),
            shape((TOK, WIDTH), F32),
            shape((12, 2, SENT, SENT), BF),
            *shards,
            shape((16, 128), F32),
        ],
        in_specs=[scalars, away, whole, whole] + [away] * 6 + [whole] * 9,
        out_specs=[whole, away, away] + [whole] * 7,
        scratch_shapes=[
            pltpu.VMEM((WIDTH, INNER), BF),
            pltpu.VMEM((WIDTH, INNER), BF),
            pltpu.VMEM((INNER, WIDTH), BF),
            pltpu.VMEM((512, 128), F32),
            pltpu.VMEM((INNER, WIDTH), BF),
            pltpu.VMEM((SLOTS, 384, 768), BF),
            pltpu.VMEM((SLOTS, 2, 96, 384), BF),
            pltpu.VMEM((SLOTS, 2, 96, 768), BF),
            pltpu.VMEM((SLOTS, 3, 24, 768), BF),
            pltpu.VMEM((TOK, INNER), BF),
            pltpu.VMEM((TOK, INNER), BF),
            pltpu.VMEM((TOK, 2304), BF),
            pltpu.VMEM((TOK, WIDTH), BF),
            pltpu.VMEM((TOK, WIDTH), BF),
            pltpu.VMEM((TOK, WIDTH), BF),
            pltpu.VMEM((TOK, WIDTH), BF),
            pltpu.VMEM((TOK, WIDTH), F32),
            pltpu.VMEM((2, 2, SENT, SENT), BF),
            pltpu.VMEM((TOK, 1), F32),
            pltpu.VMEM((TOK, 1), F32),
            pltpu.VMEM((16, INNER), F32),
            pltpu.VMEM((16, INNER), F32),
            pltpu.VMEM((8, WIDTH), F32),
            pltpu.VMEM((8, WIDTH), F32),
            pltpu.VMEM((512, 128), BF),
            pltpu.VMEM((512, 128), F32),
            pltpu.VMEM((256, 128), F32),
            pltpu.VMEM((2, 32, 128), F32),
            pltpu.VMEM((2, 64, 128), F32),
            pltpu.VMEM((3, 16, 128), F32),
            pltpu.SemaphoreType.DMA((pieces, 6)),
            pltpu.SemaphoreType.DMA((pieces,)),
            pltpu.SemaphoreType.DMA((VEC + 1, 6)),
            pltpu.SemaphoreType.DMA((VEC + 1, 2)),
            pltpu.SemaphoreType.REGULAR((SLOTS,)),
            pltpu.SemaphoreType.DMA,
            pltpu.SemaphoreType.DMA,
            pltpu.SemaphoreType.DMA((2,)),
            pltpu.SemaphoreType.DMA((4,)),
            pltpu.SemaphoreType.DMA((10,)),
            pltpu.VMEM((TOK, WIDTH), BF),
        ],
        compiler_params=pltpu.CompilerParams(
            collective_id=0, has_side_effects=True, vmem_limit_bytes=VMEM_ALL
        ),
        name="train_step",
    )(seq_lengths.reshape(2), x, pos_index, pos_count, *masters)
    loss, hidden, grads = outs[0], outs[1], outs[3:]
    vectors = [shape((size,), F32) for size in VECTOR_SIZES]
    final = pl.pallas_call(
        emit_kernel,
        out_shape=[shape((TOK, WIDTH), F32), *shards, *vectors, shape((1,), F32)],
        in_specs=[away] * 7 + [whole, scalars],
        out_specs=[away] * 7 + [whole] * 9 + [scalars],
        scratch_shapes=[pltpu.VMEM((TOK, WIDTH), F32)]
        + [pltpu.VMEM(s.shape, F32) for s in shards]
        + [pltpu.SemaphoreType.DMA((14,)), pltpu.SemaphoreType.DMA((14,))],
        name="emit",
    )(hidden, *grads[:6], grads[6], loss)
    return (final[16].reshape(()), final[0].reshape(hidden_in.shape), *final[1:16])


def device_step(mesh):
    if mesh.shape["twin"] == 2 and mesh.shape["dp"] == 16:
        return fused_device
    return staged_device


def solution(mesh):
    in_specs = (
        P("twin", "dp", None, None),
        P("twin", "dp"),
        P(),
        P(),
        P(("twin", "dp"), None),
        P(("twin", "dp"), None),
        P(("twin", "dp"), None),
        P(("twin", "dp"), None),
        P(("twin", "dp"), None),
        P(("twin", "dp"), None),
        P(("twin", "dp")),
        P(("twin", "dp")),
        P(("twin", "dp")),
        P(("twin", "dp")),
        P(("twin", "dp")),
        P(("twin", "dp")),
        P(("twin", "dp")),
        P(("twin", "dp")),
        P(("twin", "dp")),
    )
    out_specs = (
        P(),
        P("twin", "dp", None, None),
        P(("twin", "dp"), None),
        P(("twin", "dp"), None),
        P(("twin", "dp"), None),
        P(("twin", "dp"), None),
        P(("twin", "dp"), None),
        P(("twin", "dp"), None),
        P(("twin", "dp")),
        P(("twin", "dp")),
        P(("twin", "dp")),
        P(("twin", "dp")),
        P(("twin", "dp")),
        P(("twin", "dp")),
        P(("twin", "dp")),
        P(("twin", "dp")),
        P(("twin", "dp")),
    )
    return jax.shard_map(
        device_step(mesh), mesh=mesh, in_specs=in_specs, out_specs=out_specs, check_vma=False
    )
```

```python
import jax
import jax.numpy as jnp
from jax import lax
from jax.experimental import pallas as pl
from jax.experimental.pallas import tpu as pltpu
from jax.sharding import PartitionSpec as P

HEADS = 12
HDIM = 64
MICRO = 2


norm_eps = 1e-12
cosine_scale = 50.0
static_scale = 256.0


def layer_norm(values, gain_vec, shift_vec):
    center = values - jnp.mean(values, axis=-1, keepdims=True)
    spread = jnp.mean(center * center, axis=-1, keepdims=True)
    return center * lax.rsqrt(spread + norm_eps) * gain_vec + shift_vec


def exact_gelu(values):
    return jax.nn.gelu(values, approximate=False)


def product(left, right):
    return jnp.dot(left, right, preferred_element_type=jnp.float32)


def product_lt(left, right):
    return lax.dot_general(
        left, right, (((0,), (0,)), ((), ())), preferred_element_type=jnp.float32
    )


def product_rt(left, right):
    return lax.dot_general(
        left, right, (((1,), (1,)), ((), ())), preferred_element_type=jnp.float32
    )


def column_sum(values):
    return jnp.sum(values.astype(jnp.float32), axis=0)


def batch_loss(pooled_all, pos_list, pos_num):
    anchors = pooled_all.shape[0] // 2
    anchor = pooled_all[:anchors]
    positive = pooled_all[anchors:]
    anchor_n = anchor * lax.rsqrt(jnp.sum(anchor * anchor, axis=-1, keepdims=True) + 1e-06)
    positive_n = positive * lax.rsqrt(jnp.sum(positive * positive, axis=-1, keepdims=True) + 1e-06)
    sims = cosine_scale * jnp.dot(anchor_n, positive_n.T, precision=lax.Precision.HIGHEST)
    row_top = jnp.max(sims, axis=-1, keepdims=True)
    log_total = row_top[:, 0] + jnp.log(jnp.sum(jnp.exp(sims - row_top), axis=-1))
    columns = jnp.arange(anchors, dtype=jnp.int32)
    slots = jnp.arange(pos_list.shape[1], dtype=jnp.int32)
    hits = (pos_list[:, :, None] == columns[None, None, :]) & (
        slots[None, :, None] < pos_num[:, None, None]
    )
    target = jnp.sum(hits.astype(jnp.float32), axis=1) / pos_num[:, None].astype(jnp.float32)
    return jnp.sum(log_total - jnp.sum(target * sims, axis=-1))


def fetch_weights(masters):
    return (
        lax.all_gather(masters[0].astype(jnp.bfloat16), ("twin", "dp"), axis=0, tiled=True),
        lax.all_gather(masters[1].astype(jnp.bfloat16), ("twin", "dp"), axis=0, tiled=True),
        lax.all_gather(masters[2].astype(jnp.bfloat16), ("twin", "dp"), axis=0, tiled=True),
        lax.all_gather(masters[3].astype(jnp.bfloat16), ("twin", "dp"), axis=0, tiled=True),
        lax.all_gather(masters[4].astype(jnp.bfloat16), ("twin", "dp"), axis=0, tiled=True),
        lax.all_gather(masters[5].astype(jnp.bfloat16), ("twin", "dp"), axis=0, tiled=True),
        lax.all_gather(masters[6].astype(jnp.bfloat16), ("twin", "dp"), axis=0, tiled=True),
        lax.all_gather(masters[7].astype(jnp.bfloat16), ("twin", "dp"), axis=0, tiled=True),
        lax.all_gather(masters[8].astype(jnp.bfloat16), ("twin", "dp"), axis=0, tiled=True),
        lax.all_gather(masters[9].astype(jnp.bfloat16), ("twin", "dp"), axis=0, tiled=True),
        lax.all_gather(masters[10].astype(jnp.bfloat16), ("twin", "dp"), axis=0, tiled=True),
        lax.all_gather(masters[11].astype(jnp.bfloat16), ("twin", "dp"), axis=0, tiled=True),
        lax.all_gather(masters[12].astype(jnp.bfloat16), ("twin", "dp"), axis=0, tiled=True),
        lax.all_gather(masters[13].astype(jnp.bfloat16), ("twin", "dp"), axis=0, tiled=True),
        lax.all_gather(masters[14].astype(jnp.bfloat16), ("twin", "dp"), axis=0, tiled=True),
    )


def settle_grads(grad_sums):
    return (
        lax.psum_scatter(grad_sums[0], ("twin", "dp"), scatter_dimension=0, tiled=True),
        lax.psum_scatter(grad_sums[1], ("twin", "dp"), scatter_dimension=0, tiled=True),
        lax.psum_scatter(grad_sums[2], ("twin", "dp"), scatter_dimension=0, tiled=True),
        lax.psum_scatter(grad_sums[3], ("twin", "dp"), scatter_dimension=0, tiled=True),
        lax.psum_scatter(grad_sums[4], ("twin", "dp"), scatter_dimension=0, tiled=True),
        lax.psum_scatter(grad_sums[5], ("twin", "dp"), scatter_dimension=0, tiled=True),
        lax.psum_scatter(grad_sums[6], ("twin", "dp"), scatter_dimension=0, tiled=True),
        lax.psum_scatter(grad_sums[7], ("twin", "dp"), scatter_dimension=0, tiled=True),
        lax.psum_scatter(grad_sums[8], ("twin", "dp"), scatter_dimension=0, tiled=True),
        lax.psum_scatter(grad_sums[9], ("twin", "dp"), scatter_dimension=0, tiled=True),
        lax.psum_scatter(grad_sums[10], ("twin", "dp"), scatter_dimension=0, tiled=True),
        lax.psum_scatter(grad_sums[11], ("twin", "dp"), scatter_dimension=0, tiled=True),
        lax.psum_scatter(grad_sums[12], ("twin", "dp"), scatter_dimension=0, tiled=True),
        lax.psum_scatter(grad_sums[13], ("twin", "dp"), scatter_dimension=0, tiled=True),
        lax.psum_scatter(grad_sums[14], ("twin", "dp"), scatter_dimension=0, tiled=True),
    )


def masked_scores(query_heads, key_heads, live_mask):
    raw_scores = jnp.einsum(
        "sqhd,skhd->shqk", query_heads, key_heads, preferred_element_type=jnp.float32
    ) * HDIM ** (-0.5)
    return jnp.where(live_mask[:, None, None, :], raw_scores, -1000000000.0)


def forward(tokens, live_mask, pool_weight, params):
    seq_count, seq_len, width = tokens.shape
    flat = tokens.reshape(seq_count * seq_len, width)
    head_shape = (seq_count, seq_len, HEADS, HDIM)
    query_heads = (product(flat, params[0]) + params[6]).astype(jnp.bfloat16).reshape(head_shape)
    key_heads = product(flat, params[1]).astype(jnp.bfloat16).reshape(head_shape)
    value_heads = (product(flat, params[2]) + params[7]).astype(jnp.bfloat16).reshape(head_shape)
    scores = masked_scores(query_heads, key_heads, live_mask)
    row_top = jnp.max(scores, axis=-1, keepdims=True)
    exp_terms = jnp.exp(scores - row_top)
    row_total = jnp.sum(exp_terms, axis=-1, keepdims=True)
    log_total = row_top + jnp.log(row_total)
    probs_low = (exp_terms / row_total).astype(jnp.bfloat16)
    mixed = jnp.einsum(
        "shqk,skhd->sqhd", probs_low, value_heads, preferred_element_type=jnp.float32
    )
    mixed = mixed.astype(jnp.bfloat16).reshape(seq_count * seq_len, width)
    first = flat.astype(jnp.float32) + (product(mixed, params[3]) + params[8])
    normed = layer_norm(first, params[9], params[10])
    inner = product(normed.astype(jnp.bfloat16), params[4]) + params[11]
    active = exact_gelu(inner).astype(jnp.bfloat16)
    second = normed + (product(active, params[5]) + params[12])
    output = layer_norm(second, params[13], params[14])
    pooled = jnp.sum(
        output.reshape(seq_count, seq_len, width) * pool_weight[:, :, None], axis=1
    ).astype(jnp.bfloat16)
    saved = (
        query_heads,
        key_heads,
        value_heads,
        log_total,
        mixed,
        first,
        normed,
        inner,
        active,
        second,
    )
    return (pooled, saved)


def backward(tokens, live_mask, pool_weight, params, saved, pool_grad):
    query_heads, key_heads, value_heads, log_total, mixed, first, normed, inner, active, second = (
        saved
    )
    seq_count, seq_len, width = tokens.shape
    flat = tokens.reshape(seq_count * seq_len, width)
    head_shape = (seq_count, seq_len, HEADS, HDIM)
    out_grad = (pool_weight[:, :, None] * pool_grad[:, None, :]).reshape(seq_count * seq_len, width)
    unused, second_pull = jax.vjp(
        layer_norm, second, params[13].astype(jnp.float32), params[14].astype(jnp.float32)
    )
    dsecond, dgain_two, dshift_two = second_pull(out_grad)
    dffn = dsecond.astype(jnp.bfloat16)
    dshrink_bias = column_sum(dffn)
    dshrink = product_lt(active, dffn)
    dactive = product_rt(dffn, params[5])
    unused, gelu_pull = jax.vjp(exact_gelu, inner)
    dinner = gelu_pull(dactive)[0].astype(jnp.bfloat16)
    dexpand_bias = column_sum(dinner)
    dexpand = product_lt(normed.astype(jnp.bfloat16), dinner)
    dnormed = dsecond + product_rt(dinner, params[4])
    unused, first_pull = jax.vjp(
        layer_norm, first, params[9].astype(jnp.float32), params[10].astype(jnp.float32)
    )
    dfirst, dgain_one, dshift_one = first_pull(dnormed)
    dbranch = dfirst.astype(jnp.bfloat16)
    dmixer_bias = column_sum(dbranch)
    dmixer = product_lt(mixed, dbranch)
    dmixed = product_rt(dbranch, params[3]).astype(jnp.bfloat16).reshape(head_shape)
    scores = masked_scores(query_heads, key_heads, live_mask)
    probs_full = jnp.exp(scores - log_total)
    probs_low = probs_full.astype(jnp.bfloat16)
    dvalue = jnp.einsum(
        "shqk,sqhd->skhd", probs_low, dmixed, preferred_element_type=jnp.float32
    ).astype(jnp.bfloat16)
    dprobs = jnp.einsum("sqhd,skhd->shqk", dmixed, value_heads, preferred_element_type=jnp.float32)
    row_delta = jnp.sum(probs_full * dprobs, axis=-1, keepdims=True)
    dscores = (probs_full * (dprobs - row_delta)).astype(jnp.bfloat16)
    dquery = (
        jnp.einsum("shqk,skhd->sqhd", dscores, key_heads, preferred_element_type=jnp.float32)
        * HDIM ** (-0.5)
    ).astype(jnp.bfloat16)
    dkey = (
        jnp.einsum("shqk,sqhd->skhd", dscores, query_heads, preferred_element_type=jnp.float32)
        * HDIM ** (-0.5)
    ).astype(jnp.bfloat16)
    dquery = dquery.reshape(seq_count * seq_len, width)
    dkey = dkey.reshape(seq_count * seq_len, width)
    dvalue = dvalue.reshape(seq_count * seq_len, width)
    dtokens = (
        dfirst
        + product_rt(dquery, params[0])
        + product_rt(dkey, params[1])
        + product_rt(dvalue, params[2])
    )
    grad_terms = (
        product_lt(flat, dquery),
        product_lt(flat, dkey),
        product_lt(flat, dvalue),
        dmixer,
        dexpand,
        dshrink,
        column_sum(dquery),
        column_sum(dvalue),
        dmixer_bias,
        dgain_one,
        dshift_one,
        dexpand_bias,
        dshrink_bias,
        dgain_two,
        dshift_two,
    )
    return (dtokens.reshape(seq_count, seq_len, width), grad_terms)


def staged_device(
    hidden_in,
    seq_lengths,
    pos_index,
    pos_count,
    query_proj,
    key_proj,
    value_proj,
    mixer_proj,
    expand_proj,
    shrink_proj,
    query_bias,
    value_bias,
    mixer_bias,
    first_gain,
    first_shift,
    expand_bias,
    shrink_bias,
    second_gain,
    second_shift,
):
    masters = (
        query_proj,
        key_proj,
        value_proj,
        mixer_proj,
        expand_proj,
        shrink_proj,
        query_bias,
        value_bias,
        mixer_bias,
        first_gain,
        first_shift,
        expand_bias,
        shrink_bias,
        second_gain,
        second_shift,
    )
    tower = lax.axis_index("twin")
    rank = lax.axis_index("dp")
    tokens_all = hidden_in[0]
    lengths_all = seq_lengths[0]
    per_micro = tokens_all.shape[0] // MICRO
    anchors = per_micro * lax.axis_size("dp")
    seq_len = tokens_all.shape[1]
    positions = jnp.arange(seq_len, dtype=jnp.int32)
    own_start = tower * anchors + rank * per_micro
    grad_total = None
    loss_total = jnp.zeros((), jnp.float32)
    input_grads = []
    for micro_step in range(MICRO):
        params = fetch_weights(masters)
        tokens = tokens_all[micro_step * per_micro : (micro_step + 1) * per_micro]
        lengths = lengths_all[micro_step * per_micro : (micro_step + 1) * per_micro]
        live_mask = positions[None, :] < lengths[:, None]
        pool_weight = live_mask.astype(jnp.float32) / lengths[:, None].astype(jnp.float32)
        pooled, saved = forward(tokens, live_mask, pool_weight, params)
        gathered = lax.all_gather(pooled, ("twin", "dp"), axis=0, tiled=True).astype(jnp.float32)
        pos_list = pos_index[micro_step]
        pos_num = pos_count[micro_step]
        loss_part, loss_pull = jax.vjp(
            lambda values: batch_loss(values, pos_list, pos_num), gathered
        )
        gathered_grad = loss_pull(jnp.ones((), jnp.float32))[0] * static_scale
        pool_grad = lax.dynamic_slice_in_dim(gathered_grad, own_start, per_micro, 0)
        dtokens, grad_terms = backward(tokens, live_mask, pool_weight, params, saved, pool_grad)
        input_grads.append(dtokens)
        loss_total = loss_total + loss_part
        grad_total = (
            grad_terms
            if grad_total is None
            else tuple((left + right for left, right in zip(grad_total, grad_terms)))
        )
    shards = settle_grads(grad_total)
    hidden_grad = jnp.concatenate(input_grads, axis=0)[None]
    loss_value = loss_total / (MICRO * anchors)
    return (
        loss_value,
        hidden_grad,
        shards[0],
        shards[1],
        shards[2],
        shards[3],
        shards[4],
        shards[5],
        shards[6],
        shards[7],
        shards[8],
        shards[9],
        shards[10],
        shards[11],
        shards[12],
        shards[13],
        shards[14],
    )


BF = jnp.bfloat16
F32 = jnp.float32
MESH = pl.DeviceIdType.MESH
VMEM_ALL = 67043328
TOK, WIDTH, INNER, SENT = 1024, 768, 3072, 512
SLOTS = 7
QB, VB, MB, G1, S1, EB, SB, G2, S2 = range(9)
VECTOR_SIZES = (24, 24, 24, 24, 24, 96, 24, 24, 24)
PIECES = (
    [(3, 16, 0, 128)]
    + [(0, 24, 0, 384), (0, 24, 384, 384)]
    + [(0, 24, 768 * j, 768) for j in range(1, 4)]
    + [(1, 24, 768 * j, 768) for j in range(4)]
    + [(2, 96, 256 * j, 256) for j in range(3)]
)
LATE = ()
EARLY = 13
GRADS = (
    [(96, 24 * j, 0, 768) for j in range(4)]
    + [(24, 768 * j, 0, 768) for j in range(4)]
    + [(24, 0, 0, 768), (24, 768, 0, 768), (24, 1536, 0, 768)]
    + [(24, 2304, 0, 384), (24, 2304, 384, 384)]
)
VEC = len(GRADS)

AHEAD = 5
FORWARD = {'attend0': {0: ('g2', 'k5', 'a10'),
             1: ('k6', 'a11', 'i4'),
             2: ('g3',),
             3: ('k7', 'a12')},
 'attend1': {0: ('k8',), 1: ('i6',), 2: ('k9', 'g4')},
 'attend2': {0: ('g5',), 2: ('f5', 'i8', 'k11'), 3: ('g6',)},
 'exp0': {0: ('g7',), 4: ('f7', 'i10')},
 'exp1': {0: ('g8',), 4: ('f8', 'i11')},
 'exp2': {2: ('i12',), 4: ('g9',)},
 'exp3': {-1: ('g10', 'f9'), 2: ('f10', 'g11'), 5: ('g12',)},
 'mix': {1: ('k12', 'i9'), 3: ('f6',)},
 'proj0': {-1: ('f1',), 1: ('i3',)},
 'proj1': {-1: ('i5', 'f3')},
 'proj2': {-1: ('i7', 'f4'), 1: ('k10',)},
 'projh': {-1: ('f2',)},
 'shr0': {0: ('f11',)},
 'shr2': {-1: ('f12',)},
 'vec': {-1: ('k0',
              'a5',
              'k1',
              'a6',
              'k2',
              'a7',
              'i0',
              'i1',
              'k3',
              'a8',
              'i2',
              'g0',
              'k4',
              'a9',
              'g1',
              'f0')}}
BACKWARD = {'actb': {3: ('c0', 'r0'),
          4: ('c1', 'r1', 'c2', 'r2'),
          5: ('c3', 'r3'),
          8: ('d0',),
          10: ('d1',)},
 'attb0': {0: ('s5', 'c8', 'r8'), 1: ('d7',), 2: ('s6',), 3: ('f4', 'd8')},
 'attb1': {1: ('f6', 's8', 'c9', 'r9'), 3: ('f7',)},
 'attb2': {0: ('f8',), 1: ('c10', 'r10'), 3: ('d10', 'c11', 'r11')},
 'expg0': {0: ('d2',), 2: ('d3',)},
 'expg2': {0: ('s0',), 1: ('c4', 'r4')},
 'expg3': {0: ('c5', 's1', 'r5')},
 'firstb': {0: ('s3',), 1: ('f1', 'd4', 'd5', 'c7', 'r7'), 2: ('f2', 'd6')},
 'inb': {0: ('c12', 'r12'),
         1: ('s10', 'c13', 'r13'),
         2: ('d11',),
         4: ('d12', 'd13')},
 'ing0': {2: ('f5', 's7')},
 'ing1': {0: ('d9',)},
 'ingh0': {0: ('s9',)},
 'mixb': {0: ('f3', 's4')},
 'st7': {-1: ('c6', 'r6', 's2', 'f0')},
 'tail': {-1: ('s11', 's12', 'f10', 's13', 'f11', 'f12', 'f13')},
 'tiles': {2: ('f9',)}}


def coords():
    rank = lax.axis_index("dp")
    return lax.axis_index("twin"), rank // 4, (rank // 2) % 2, rank % 2


def flat(t, z, y, c):
    return t * 16 + z * 4 + y * 2 + c


def dev(t, z, y, c):
    return {"twin": t, "dp": z * 4 + y * 2 + c}


def neighbours(t, z, y, c):
    return [dev(t, (z + k) % 4, y, c) for k in (1, 2, 3)] + [
        dev(1 - t, z, y, c),
        dev(t, z, 1 - y, c),
        dev(t, z, y, 1 - c),
    ]


def signal_all(sem):
    for other in neighbours(*coords()):
        pl.semaphore_signal(sem, inc=1, device_id=other, device_id_type=MESH)


def send(src, dst, send_sem, recv_sem, target):
    pltpu.make_async_remote_copy(
        src, dst, send_sem, recv_sem, device_id=target, device_id_type=MESH
    ).start()


def wait_bytes(ref, sem):
    pltpu.make_async_copy(ref, ref, sem).wait()


class Gather:
    def __init__(self, arrays, recv, sent):
        self.arrays, self.recv, self.sent = arrays, recv, sent
        self.at = coords()

    def rows(self, p, owner):
        w, r, c0, nc = PIECES[p]
        return self.arrays[w].at[pl.ds(pl.multiple_of(owner * r, 8), r), pl.ds(c0, nc)]

    def halves(self, p, owners, half):
        w, r, c0, nc = PIECES[p]
        if nc % 256:
            return [self.rows(p, owner) for owner in owners[2 * half : 2 * half + 2]]
        cols = pl.ds(c0 + half * (nc // 2), nc // 2)
        return [
            self.arrays[w].at[pl.ds(pl.multiple_of(owner * r, 8), r), cols] for owner in owners
        ]

    def put(self, p, part, target, group):
        send(part, part, self.sent.at[p], self.recv.at[p, group], target)

    def wait(self, p, group, shards):
        w, r, c0, nc = PIECES[p]
        wait_bytes(
            self.arrays[w].at[pl.ds(0, shards * r), pl.ds(c0, nc)], self.recv.at[p, group]
        )

    def start(self, p):
        t, z, y, c = self.at
        own = self.rows(p, flat(t, z, y, c))
        self.along_z(p, own)
        if p < EARLY or p in LATE:
            self.across(p, own)

    def across(self, p, part):
        t, z, y, c = self.at
        self.put(p, part, dev(1 - t, z, y, c), 1)
        self.put(p, part, dev(t, z, 1 - y, c), 2)
        self.put(p, part, dev(t, z, y, 1 - c), 5)

    def along_z(self, p, part):
        t, z, y, c = self.at
        for k in (1, 2, 3):
            self.put(p, part, dev(t, (z + k) % 4, y, c), 0)

    def column(self, p):
        t, z, y, c = self.at
        if p in LATE:
            self.wait(p, 0, 12)
            for k in (1, 2, 3):
                for tt in range(2):
                    for yy in range(2):
                        part = self.rows(p, flat(tt, (z + k) % 4, yy, c))
                        self.put(p, part, dev(t, z, y, 1 - c), 5)
            return
        self.wait(p, 0, 3)
        for k in range(1 if p < EARLY else 0, 4):
            self.across(p, self.rows(p, flat(t, (z + k) % 4, y, c)))

    def sides(self, p):
        t, z, y, c = self.at
        steps = [z] if p in LATE else range(4)
        self.wait(p, 1, len(steps))
        owners = [flat(1 - t, k, y, c) for k in steps]
        for part in self.halves(p, owners, 0):
            self.put(p, part, dev(t, z, 1 - y, c), 4)
        for owner in owners:
            self.put(p, self.rows(p, owner), dev(t, z, y, 1 - c), 5)
            if p in LATE:
                self.along_z(p, self.rows(p, owner))
        self.wait(p, 2, len(steps))
        owners = [flat(t, k, 1 - y, c) for k in steps]
        for part in self.halves(p, owners, 1):
            self.put(p, part, dev(1 - t, z, y, c), 3)
        for owner in owners:
            self.put(p, self.rows(p, owner), dev(t, z, y, 1 - c), 5)
            if p in LATE:
                self.along_z(p, self.rows(p, owner))

    def diagonal(self, p):
        t, z, y, c = self.at
        owners = [flat(1 - t, k, 1 - y, c) for k in ([z] if p in LATE else range(4))]
        for group, half in ((3, 1), (4, 0)):
            if p in LATE:
                part = self.halves(p, owners, half)[0]
                wait_bytes(part, self.recv.at[p, group])
                self.along_z(p, part)
            else:
                self.wait(p, group, 2)
            for part in self.halves(p, owners, half):
                self.put(p, part, dev(t, z, y, 1 - c), 5)

    def finish(self, p):
        self.wait(p, 5, 16)

    def drain(self, p):
        w, r, c0, nc = PIECES[p]
        wait_bytes(self.arrays[w].at[pl.ds(0, 31 * r), pl.ds(c0, nc)], self.sent.at[p])

    def table(self):
        return {
            "a": self.start,
            "k": self.column,
            "i": self.sides,
            "g": self.diagonal,
            "f": self.finish,
        }


class Scatter:
    def __init__(self, grad, bufs, vec_grad, vec_bufs, recv, sent, free, store):
        self.grad, self.bufs, self.vec_grad, self.vec_bufs = grad, bufs, vec_grad, vec_bufs
        self.recv, self.sent, self.free, self.store = recv, sent, free, store
        self.at = coords()

    def size(self, p):
        return (16, 128) if p == VEC else (24, GRADS[p][3])

    def buf(self, p, which):
        if p == VEC:
            return self.vec_bufs[which]
        whole = self.bufs[which].at[p % SLOTS]
        if GRADS[p][3] == 768:
            return whole
        cols = pl.ds(0, 384)
        if which == 0:
            return whole.at[:, cols]
        if which == 1:
            return whole.at[:, pl.ds(0, 48), :]
        return whole.at[:, :, cols]

    def part(self, p, owner):
        if p == VEC:
            return self.vec_grad.at[pl.ds(pl.multiple_of(owner * 16, 8), 16), :]
        stride, base, col, cols = GRADS[p]
        return self.grad.at[
            pl.ds(pl.multiple_of(owner * stride + base, 8), 24), pl.ds(col, cols)
        ]

    def mine(self, p, t, z, y, n=1):
        r, nc = self.size(p)
        first = pl.multiple_of((t * 8 + y * 4 + z) * r, 8)
        return self.buf(p, 0).at[pl.ds(first, n * r), :]

    def half(self, p, t, y, half):
        r, nc = self.size(p)
        first = (t * 8 + y * 4) * r
        if nc < 768:
            first = pl.multiple_of(first + half * 2 * r, 8)
            return self.buf(p, 0).at[pl.ds(first, 2 * r), :]
        return self.buf(p, 0).at[
            pl.ds(pl.multiple_of(first, 8), 4 * r), pl.ds(half * (nc // 2), nc // 2)
        ]

    def put(self, p, group, src, dst, target, lane=1):
        send(src, dst, self.sent.at[p, lane], self.recv.at[p, group], target)

    def start(self, p):
        t, z, y, c = self.at
        if SLOTS <= p < VEC:
            pl.semaphore_wait(self.free.at[p % SLOTS], 6)

        def body(i, carry):
            tt, yy, zz = i // 8, (i // 4) % 2, i % 4
            src = self.part(p, flat(tt, zz, yy, 1 - c))
            self.put(p, 0, src, self.mine(p, tt, zz, yy), dev(t, z, y, 1 - c), 0)
            return carry

        lax.fori_loop(0, 16, body, 0)

    def add_columns(self, p, first, last):
        t, z, y, c = self.at

        def body(i, carry):
            tt = (t + 1 - i // 8) % 2
            yy = (y + 1 - (i // 4) % 2) % 2
            a = self.mine(p, tt, i % 4, yy)
            b = self.part(p, flat(tt, i % 4, yy, c))
            a[...] = a[...] + b[...]
            return carry

        lax.fori_loop(first, last, body, 0)

    def cores(self, p):
        t, z, y, c = self.at
        wait_bytes(self.buf(p, 0), self.recv.at[p, 0])
        self.add_columns(p, 0, 4)
        diag = self.buf(p, 1)
        self.put(p, 2, self.half(p, 1 - t, 1 - y, 0), diag.at[0], dev(t, z, 1 - y, c))
        self.put(p, 1, self.half(p, 1 - t, 1 - y, 1), diag.at[1], dev(1 - t, z, y, c))
        self.add_columns(p, 4, 16)

    def add(self, a, b):
        a[...] = a[...] + b[...]

    def diagonals(self, p):
        t, z, y, c = self.at
        diag, side = self.buf(p, 1), self.buf(p, 2)
        wait_bytes(diag.at[0], self.recv.at[p, 2])
        self.add(self.half(p, 1 - t, y, 0), diag.at[0])
        self.put(p, 3, self.mine(p, 1 - t, 0, y, 4), side.at[0], dev(1 - t, z, y, c))
        wait_bytes(diag.at[1], self.recv.at[p, 1])
        self.add(self.half(p, t, 1 - y, 1), diag.at[1])
        self.put(p, 4, self.mine(p, t, 0, 1 - y, 4), side.at[1], dev(t, z, 1 - y, c))

    def sides(self, p):
        t, z, y, c = self.at
        side, col = self.buf(p, 2), self.buf(p, 3)
        wait_bytes(side.at[0], self.recv.at[p, 3])
        wait_bytes(side.at[1], self.recv.at[p, 4])
        a = self.mine(p, t, 0, y, 4)
        total = a[...].astype(F32) + side[0].astype(F32) + side[1].astype(F32)
        a[...] = total.astype(a.dtype)
        for k in (1, 2, 3):
            zz = (z + k) % 4
            self.put(p, 5, self.mine(p, t, zz, y), col.at[k - 1], dev(t, zz, y, c))

    def finish(self, p):
        t, z, y, c = self.at
        col = self.buf(p, 3)
        wait_bytes(col, self.recv.at[p, 5])
        total = self.mine(p, t, z, y)[...].astype(F32)
        for k in range(3):
            total = total + col[k].astype(F32)
        self.store(p, total)
        self.drain(p)
        if p + SLOTS < VEC:
            signal_all(self.free.at[p])

    def drain(self, p):
        r, nc = self.size(p)
        wait_bytes(self.buf(p, 0).at[pl.ds(0, 15 * r), :], self.sent.at[p, 1])

    def table(self):
        return {
            "c": self.cores,
            "d": self.diagonals,
            "s": self.sides,
            "f": self.finish,
            "r": self.release,
        }

    def release(self, p):
        wait_bytes(self.buf(p, 0), self.sent.at[p, 0])


def dot(a, b):
    return jnp.dot(a, b, preferred_element_type=F32)


def dot_lt(a, b):
    return lax.dot_general(a, b, (((0,), (0,)), ((), ())), preferred_element_type=F32)


def dot_rt(a, b):
    return lax.dot_general(a, b, (((1,), (1,)), ((), ())), preferred_element_type=F32)


def block(i, n):
    return pl.ds(pl.multiple_of(i * n, n), n)


def iota(shape, axis):
    return lax.broadcasted_iota(jnp.int32, shape, axis)


def loop(n, body, ticks=()):
    ticks = {k: v for k, v in dict(ticks).items() if k >= 0}

    def step(i, carry):
        body(i)
        for k, tick in ticks.items():

            @pl.when(i == k)
            def _(tick=tick):
                for part in tick:
                    part()

        return carry

    lax.fori_loop(0, n, step, 0)


def ticks_of(plan, name, table):
    return {
        k: [lambda n=n: table[n[0]](int(n[1:])) for n in names]
        for k, names in plan.get(name, {}).items()
    }


def owner_of(n, size):
    owner = jnp.floor((n.astype(F32) + 0.5) * (1.0 / size)).astype(jnp.int32)
    return owner, n - owner * size


def picks(size, first):
    width = 256
    owner, place = owner_of(first + iota((1, width), 1), size)
    return (
        jnp.where(iota((128, width), 0) == place, 1.0, 0.0).astype(BF),
        jnp.where(iota((32, width), 0) == owner, 1.0, 0.0).astype(BF),
    )


def vector_rows(vec, par, names, pick, mine):
    width = pick.shape[1]
    shards = [vec[pl.ds(k, 32, stride=16), :].astype(BF) for k in names]
    spreaded = dot(jnp.concatenate(shards, axis=0), pick)
    for i, k in enumerate(names):
        part = spreaded[32 * i : 32 * i + 32] * mine.astype(F32)
        par[k : k + 1, 0:width] = jnp.sum(part, axis=0, keepdims=True)


def vector_tiles(row, k):
    size = VECTOR_SIZES[k]
    width = 32 * size
    owner, place = owner_of(iota((1, width), 1), size)
    pick = jnp.where(iota((128, width), 0) == place, 1.0, 0.0)
    parts = jnp.where(iota((32, width), 0) == owner, row, 0.0)
    return lax.dot_general(
        parts,
        pick,
        (((1,), (1,)), ((), ())),
        precision=lax.Precision.HIGHEST,
        preferred_element_type=F32,
    )


def normalize(v):
    center = v - jnp.mean(v, axis=1, keepdims=True)
    spread_ = jnp.mean(center * center, axis=1, keepdims=True)
    scale = lax.rsqrt(spread_ + norm_eps)
    return center * scale, scale


def targets(pos, cnt):
    goals = []
    eye16 = iota((16, 16), 0) == iota((16, 16), 1)
    eye32 = jnp.where(iota((32, 32), 0) == iota((32, 32), 1), 1.0, 0.0).astype(BF)
    for m in range(MICRO):
        number = cnt[m : m + 1, :]
        hits = jnp.zeros((32, 16), F32)
        for k in range(6):
            hit = (pos[k, m : m + 1, :] + 16 == iota((32, 16), 0)) & (k < number)
            hits = hits + jnp.where(hit, 1.0, 0.0)
        hits = dot_lt(hits.astype(BF), eye32)
        number = jnp.sum(jnp.where(eye16, number, 0), axis=1, keepdims=True)
        goals.append(
            jnp.concatenate([hits / number.astype(F32), jnp.zeros((16, 32), F32)], axis=0)
        )
    return goals


def contrast(pool, goals, dpool, own):
    total = jnp.zeros((1, 1), F32)
    row, col = iota((32, 32), 0), iota((32, 32), 1)
    valid = (row < 16) & (col >= 16)
    eye = row == col
    for m in range(MICRO):
        chunks = [pool[pl.ds(8 * m + k, 32, stride=16), :] for k in range(6)]
        gram = jnp.zeros((32, 32), F32)
        for chunk in chunks:
            gram = gram + dot_rt(chunk.astype(BF), chunk.astype(BF))
        diag = jnp.where(eye, gram, 0.0)
        scale_c = lax.rsqrt(jnp.sum(diag, axis=1, keepdims=True) + 1e-6)
        scale_r = lax.rsqrt(jnp.sum(diag, axis=0, keepdims=True) + 1e-6)
        sims = cosine_scale * gram * scale_c * scale_r
        top = jnp.max(jnp.where(valid, sims, -1e30), axis=1, keepdims=True)
        terms = jnp.where(valid, jnp.exp(jnp.minimum(sims - top, 0.0)), 0.0)
        row_sum = jnp.where(row[:, :1] < 16, jnp.sum(terms, axis=1, keepdims=True), 1.0)
        logs = jnp.where(row[:, :1] < 16, top + jnp.log(row_sum), 0.0)
        target = goals[m]
        loss = logs - jnp.sum(target * sims, axis=1, keepdims=True)
        total = total + jnp.sum(jnp.where(row[:, :1] < 16, loss, 0.0), axis=0, keepdims=True)
        grad = (terms / row_sum - target) * static_scale
        mine_r = jnp.sum(jnp.where(row == own, grad * scale_r, 0.0), axis=0, keepdims=True)
        weight = jnp.sum(jnp.where(eye, mine_r, 0.0), axis=1, keepdims=True)
        weight = weight + jnp.sum(
            jnp.where(col == own, grad * scale_c, 0.0), axis=1, keepdims=True
        )
        weight = cosine_scale * weight
        mine = iota((32, 1), 0) == own
        scale = jnp.sum(jnp.where(mine, scale_c, 0.0), axis=0, keepdims=True)
        along = jnp.zeros((1, 1), F32)
        pulls = []
        for chunk in chunks:
            pull = jnp.sum(weight * chunk, axis=0, keepdims=True)
            x = jnp.sum(jnp.where(mine, chunk, 0.0), axis=0, keepdims=True)
            along = along + jnp.sum(pull * x, axis=1, keepdims=True)
            pulls.append((pull, x))
        for k, (pull, x) in enumerate(pulls):
            dpool[m : m + 1, 128 * k : 128 * k + 128] = scale * pull - x * (
                scale * scale * scale * along
            )
    return total


def step_kernel(*refs):
    (lens, tokens, pos, cnt, mq, mk, mv, mm, me, ms) = refs[:10]
    mvec = refs[10:19]
    (loss, hidden, probs, gq, gk, gv, gm, ge, gs, gvec) = refs[19:29]
    (wa, we, ws, vec, grad, rc, rd, rs, rz, act, gp, qkv, mixed, nb, n1, n2) = refs[29:45]
    (f1, pbuf, r1, r2, par, pgrad, nbar, dpool, pool) = refs[45:54]
    (vc, vd, vs, vz) = refs[54:58]
    vgrad = poolf = vec
    (g_recv, g_sent, s_recv, s_sent, free, pool_recv, pool_sent, p_sem, h_sem, in_sem, x) = refs[58:]
    t, z, y, c = coords()
    own = flat(t, z, y, c)
    gather = Gather((wa, we, ws, vec), g_recv, g_sent)

    rows = (0, 24, 48, 72, 192, 216, 240, 264, 96)
    wide = [me.at[:, pl.ds(768 * j, 768)] for j in range(4)]
    loads = [
        pltpu.make_async_copy(shard, f1.at[pl.ds(row, shard.shape[0]), :], in_sem.at[k])
        for k, (row, shard) in enumerate(zip(rows, [mq, mk, mv, mm, *wide, ms]))
    ]
    loads.append(pltpu.make_async_copy(tokens, x, in_sem.at[9]))
    for load in loads:
        load.start()
    barrier = pltpu.get_barrier_semaphore()
    signal_all(barrier)
    here24 = pl.ds(pl.multiple_of(own * 24, 8), 24)
    here16 = pl.ds(pl.multiple_of(own * 16, 8), 16)
    vec[here16, :] = jnp.zeros((16, 128), F32)
    for k, size in enumerate(VECTOR_SIZES):
        vec[pl.ds(own * 16 + k, 1), 0:size] = (
            mvec[k][...].reshape(1, size).astype(BF).astype(F32)
        )
    pl.semaphore_wait(barrier, 6)
    gather.start(0)
    for load in loads[:3]:
        load.wait()
    for g in range(6):
        for j in range(3):
            first = 384 * g + 128 * j
            shard = f1[24 * j : 24 * j + 24, 128 * g : 128 * g + 128]
            wa[here24, first : first + 128] = shard.astype(BF)
        if g in (0, 1, 3, 5):
            gather.start((g + 3) // 2 if g else 1)
    for load in loads[3:9]:
        load.wait()
    wa[here24, 2304:3072] = f1[72:96, :].astype(BF)
    for j in range(4):
        we[here24, 768 * j : 768 * j + 768] = f1[192 + 24 * j : 216 + 24 * j, :].astype(BF)
    ws[pl.ds(pl.multiple_of(own * 96, 8), 96), :] = f1[96:192, :].astype(BF)
    for p in range(5, AHEAD):
        gather.start(p)

    def planned(name):
        ticks = ticks_of(FORWARD, name, gather.table())
        for part in ticks.get(-1, ()):
            part()
        return ticks

    for ref, size, blocks in ((gp, 24, 3), (act, 96, 12)):

        def pick(i, ref=ref, size=size):
            ref[0:128, block(i, 256)], ref[128:160, block(i, 256)] = picks(size, 256 * i)

        loop(blocks, pick)
    ticks = planned("vec")
    small = [k for k in range(9) if k != EB]
    vector_rows(vec, par, small, gp[0:128, 0:768], gp[128:160, 0:768])
    for part in ticks.get(0, ()):
        part()
    vector_rows(vec, par, [EB], act[0:128, :], act[128:160, :])
    for part in ticks.get(1, ()):
        part()
    for g in range(6):
        lanes, first = slice(128 * g, 128 * g + 128), 384 * g
        par[9:10, first : first + 128] = par[QB : QB + 1, lanes] * HDIM ** (-0.5)
        par[9:10, first + 128 : first + 256] = jnp.zeros((1, 128), F32)
        par[9:10, first + 256 : first + 384] = par[VB : VB + 1, lanes]
        par[10:11, first : first + 128] = jnp.full((1, 128), HDIM ** (-0.5), F32)
        par[10:11, first + 128 : first + 384] = jnp.ones((1, 256), F32)
    loads[9].wait()

    first_head = iota((SENT, 128), 1) < 64

    def put_probs(slot, item):
        return pltpu.make_async_copy(pbuf.at[slot], probs.at[item], p_sem.at[slot])

    def project(first, size, blocks):
        def body(i):
            rows = block(i // blocks, 512)
            cols = pl.ds(pl.multiple_of(first + i % blocks * size, 128), size)
            value = dot(x[rows, :], wa[:, cols])
            qkv[rows, cols] = (value * par[10:11, cols] + par[9:10, cols]).astype(BF)

        return body

    def second_half():
        loop(2, project(384, 384, 1), planned("projh"))

    def triple(pair):
        return [pl.ds(pl.multiple_of(384 * pair + 128 * n, 128), 128) for n in range(3)]

    def attend(g):
        def body(i):
            item = 4 * g + i
            s, j = i % 2, i // 2
            slot = item % 2
            rows = block(s, SENT)
            live = iota((1, SENT), 1) < lens[s]
            if g:
                put_probs(slot, item - 2).wait()
            else:

                @pl.when(i >= 2)
                def _():
                    put_probs(slot, item - 2).wait()

            q, k, v = [qkv[rows, cols] for cols in triple(2 * g + j)]
            zero = jnp.zeros_like(q)
            outs = []
            for h in range(2):
                qh = jnp.where(first_head if h == 0 else ~first_head, q, zero)
                scores = jnp.where(live, dot_rt(qh, k), -1000000000.0)
                terms = jnp.exp(scores - jnp.max(scores, axis=1, keepdims=True))
                low = (terms * (1.0 / jnp.sum(terms, axis=1, keepdims=True))).astype(BF)
                pbuf[slot, h] = low
                outs.append(dot(low, v))
            mixed[rows, block(2 * g + j, 128)] = jnp.where(first_head, outs[0], outs[1]).astype(BF)
            put_probs(slot, item).start()

        return body

    for g in range(3):
        if g == 0:
            loop(2, project(0, 384, 1), planned("proj0"))
        else:
            loop(6, project(768 * g, 256, 3), planned("proj%d" % g))
        ticks = planned("attend%d" % g)
        if g == 0:
            ticks.setdefault(1, []).append(second_half)
        loop(4, attend(g), ticks)
    for item in (10, 11):
        put_probs(item % 2, item).wait()

    def mix(i):
        rows = block(i, 256)
        first = dot(mixed[rows, :], wa[:, 2304:3072]) + par[MB : MB + 1, 0:768]
        n, r = normalize(x[rows, :].astype(F32) + first)
        n1[rows, :] = n.astype(BF)
        r1[rows, :] = r
        normed = n * par[G1 : G1 + 1, 0:768] + par[S1 : S1 + 1, 0:768]
        f1[rows, :] = normed
        nb[rows, :] = normed.astype(BF)

    loop(4, mix, planned("mix"))

    for j in range(4):

        def expand(i, j=j):
            rows, cols = block(i % 2, 512), block(3 * j + i // 2, 256)
            v = dot(nb[rows, :], we[:, cols]) + par[EB : EB + 1, cols]
            phi = 0.5 + 0.5 * lax.erf(v * 0.7071067811865476)
            act[rows, cols] = (v * phi).astype(BF)
            slope = phi + v * (jnp.exp(-0.5 * (v * v)) * 0.3989422804014327)
            gp[rows, cols] = slope.astype(BF)

        loop(6, expand, planned("exp%d" % j))
    for j in range(3):

        def shrink(i, j=j):
            rows, cols = block(i, 512), slice(256 * j, 256 * j + 256)
            value = dot(act[rows, :], ws[:, cols]) + par[SB : SB + 1, cols]
            f1[rows, cols] = f1[rows, cols] + value

        loop(2, shrink, planned("shr%d" % j))

    nbar[...] = jnp.zeros_like(nbar)

    def weight_of(i, n):
        s = (i * n) // SENT
        length = lens[s]
        token = iota((n, 1), 0) + (i * n - s * SENT)
        return jnp.where(token < length, 1.0, 0.0) / length.astype(F32)

    def finish_norm(i):
        rows = block(i, 128)
        n, r = normalize(f1[rows, :])
        w = weight_of(i, 128)
        n2[rows, :] = n.astype(BF)
        r2[rows, :] = r * w
        total = jnp.sum(n * w, axis=0, keepdims=True)
        s = i // 4
        nbar[pl.ds(s, 1), :] = nbar[pl.ds(s, 1), :] + total

    loop(8, finish_norm)
    pooled = nbar[0:2, :] * par[G2 : G2 + 1, 0:768] + par[S2 : S2 + 1, 0:768]
    tile = jnp.zeros((16, 128), F32)
    place = iota((16, 128), 0)
    for m in range(2):
        for k in range(6):
            tile = jnp.where(place == 8 * m + k, pooled[m : m + 1, 128 * k : 128 * k + 128], tile)
    at = pool.at[pl.ds(pl.multiple_of(own * 16, 8), 16), :]
    at[...] = tile.astype(BF)

    def spread_pool(i, carry):
        other = lax.rem(own + i, 32)
        target = {"twin": other // 16, "dp": lax.rem(other, 16)}
        send(at, at, pool_sent, pool_recv, target)
        return carry

    lax.fori_loop(1, 32, spread_pool, 0)
    for p in range(len(PIECES)):
        gather.drain(p)
    goals = targets(pos, cnt)
    wait_bytes(pool.at[pl.ds(0, 496), :], pool_recv)
    poolf[...] = pool[...].astype(F32)
    loss[...] = contrast(poolf, goals, dpool, own) / (MICRO * 16)
    wait_bytes(pool.at[pl.ds(0, 496), :], pool_sent)

    def store(p, total):
        if p == VEC:
            gvec[...] = total
        elif p < 4:
            gs[24 * p : 24 * p + 24, :] = total
        elif p < 8:
            ge[:, 768 * (p - 4) : 768 * (p - 4) + 768] = total
        elif p == 8:
            gm[...] = total
        else:
            for j in range(total.shape[1] // 384):
                pair = 2 * (p - 9) + j if p < 11 else p - 7
                for n, ref in enumerate((gq, gk, gv)):
                    first = 384 * j + 128 * n
                    ref[:, 128 * pair : 128 * pair + 128] = total[:, first : first + 128]

    scatter = Scatter(
        grad, (rc, rd, rs, rz), vgrad, (vc, vd, vs, vz), s_recv, s_sent, free, store
    )
    pgrad[...] = jnp.zeros_like(pgrad)
    gain2 = par[G2 : G2 + 1, 0:768]
    pgrad[G2 : G2 + 1, 0:768] = jnp.sum(dpool[0:2, :] * nbar[0:2, :], axis=0, keepdims=True)
    pgrad[S2 : S2 + 1, 0:768] = jnp.sum(dpool[0:2, :], axis=0, keepdims=True)

    def collect(k, value):
        cols = slice(0, 32 * VECTOR_SIZES[k])
        pgrad[k : k + 1, cols] = pgrad[k : k + 1, cols] + jnp.sum(value, axis=0, keepdims=True)

    def second_back(i):
        rows = block(i, 128)
        u = dpool[pl.ds(i // 4, 1), :] * gain2
        u = u - jnp.mean(u, axis=1, keepdims=True)
        n = n2[rows, :].astype(F32)
        along = jnp.mean(n * u, axis=1, keepdims=True)
        back = r2[rows, :] * (u - n * along)
        f1[rows, :] = back
        low = back.astype(BF)
        n2[rows, :] = low
        collect(SB, low.astype(F32))

    loop(8, second_back)

    def shrink_grad(i):
        grad[block(i, 256), :] = dot_lt(act[:, block(i, 256)], n2[...]).astype(BF)

    loop(12, shrink_grad)
    for p in range(4):
        scatter.start(p)

    def planned(name):
        ticks = ticks_of(BACKWARD, name, scatter.table())
        for part in ticks.get(-1, ()):
            part()
        return ticks

    def act_back(i):
        cols = block(i, 256)
        back = dot_rt(n2[...], ws[cols, :]) * gp[:, cols].astype(F32)
        low = back.astype(BF)
        gp[:, cols] = low
        pgrad[EB : EB + 1, cols] = jnp.sum(low.astype(F32), axis=0, keepdims=True)

    loop(12, act_back, planned("actb"))
    planned("expg")

    def expand_grad(i, j):
        cols = block(3 * j + i, 256)
        grad[768 * j : 768 * j + 768, block(i, 256)] = dot_lt(nb[...], gp[:, cols]).astype(BF)

    for j in range(4):
        loop(3, lambda i, j=j: expand_grad(i, j), planned("expg%d" % j))
        planned("st%d" % (4 + j))
        scatter.start(4 + j)

    def first_back(i):
        rows = block(i, 256)
        back = f1[rows, :] + dot_rt(gp[rows, :], we[...])
        n = n1[rows, :].astype(F32)
        collect(G1, back * n)
        collect(S1, back)
        dn = back * par[G1 : G1 + 1, 0:768]
        mean = jnp.mean(dn, axis=1, keepdims=True)
        along = jnp.mean(dn * n, axis=1, keepdims=True)
        back = r1[rows, :] * (dn - mean - n * along)
        f1[rows, :] = back
        low = back.astype(BF)
        n2[rows, :] = low
        collect(MB, low.astype(F32))

    loop(4, first_back, planned("firstb"))

    def mixer_grad(i):
        grad[0:768, block(i, 256)] = dot_lt(mixed[...], n2[:, block(i, 256)]).astype(BF)

    loop(3, mixer_grad, planned("mixg"))
    planned("st8")
    scatter.start(8)

    def get_probs(item):
        return pltpu.make_async_copy(probs.at[item], pbuf.at[item % 2], p_sem.at[item % 2])

    get_probs(0).start()
    get_probs(1).start()

    def mixed_back(i):
        rows = block(i, 512)
        n2[rows, :] = dot_rt(n2[rows, :], wa[:, 2304:3072]).astype(BF)

    loop(2, mixed_back, planned("mixb"))
    planned("att")

    for g in range(3):

        def attend_back(i, g=g):
            s, j = i % 2, i // 2
            pair = 2 * g + j
            item = 4 * g + i
            slot = i % 2
            rows = block(s, SENT)
            get_probs(item).wait()
            q, k, v = [qkv[rows, cols] for cols in triple(pair)]
            do = n2[rows, block(pair, 128)]
            zero = jnp.zeros_like(do)
            both = do.astype(F32) * mixed[rows, block(pair, 128)].astype(F32)
            parts = []
            for h in range(2):
                head = first_head if h == 0 else ~first_head
                p = pbuf[slot, h]
                delta = jnp.sum(jnp.where(head, both, 0.0), axis=1, keepdims=True)
                dp = dot_rt(jnp.where(head, do, zero), v)
                ds = (p.astype(F32) * (dp - delta)).astype(BF)
                parts.append((dot(ds, k) * (HDIM ** (-0.5)), dot_lt(ds, q), dot_lt(p, do)))
            for n, cols in enumerate(triple(pair)):
                value = jnp.where(first_head, parts[0][n], parts[1][n])
                act[rows, cols] = value.astype(BF)

            @pl.when(item + 2 < 12)
            def _():
                get_probs(item + 2).start()

        def half_grad(j):
            def body(i):
                cols = pl.ds(1536 + 384 * j, 384)
                grad[pl.ds(pl.multiple_of(2304 + 384 * i, 8), 384), 384 * j : 384 * j + 384] = (
                    dot_lt(x[:, block(i, 384)], act[:, cols]).astype(BF)
                )

            loop(2, body, planned("ingh%d" % j))
            planned("st%d" % (11 + j))
            scatter.start(11 + j)

        def input_grad(i, g=g):
            grad[768 * (g + 1) : 768 * (g + 2), block(i, 256)] = dot_lt(
                x[...], act[:, block(3 * g + i, 256)]
            ).astype(BF)

        ticks = planned("attb%d" % g)
        if g == 2:
            ticks.setdefault(1, []).append(lambda: half_grad(0))
        loop(4, attend_back, ticks)
        if g == 2:
            half_grad(1)
        else:
            loop(3, input_grad, planned("ing%d" % g))
            planned("st%d" % (9 + g))
            scatter.start(9 + g)
        for j in range(2):
            first, lanes = 768 * g + 384 * j, slice(256 * g + 128 * j, 256 * g + 128 * j + 128)
            for k, col in ((QB, first), (VB, first + 256)):
                pgrad[k : k + 1, lanes] = jnp.sum(
                    act[:, col : col + 128].astype(F32), axis=0, keepdims=True
                )
    ticks = planned("tiles")
    for k in range(9):
        tiles = vector_tiles(pgrad[k : k + 1, 0 : 32 * VECTOR_SIZES[k]], k)
        vgrad[pl.ds(k, 32, stride=16), :] = tiles
        if k % 3 == 2:
            for part in ticks.get(k // 3, ()):
                part()
    scatter.start(VEC)

    def put_hidden(i):
        at = (block(i // 3, 512), block(i % 3, 256))
        return pltpu.make_async_copy(f1.at[at], hidden.at[at], h_sem.at[i])

    def input_back(i):
        rows, cols = block(i // 3, 512), block(i % 3, 256)
        f1[rows, cols] = f1[rows, cols] + dot_rt(act[rows, 0:2304], wa[cols, 0:2304])
        put_hidden(i).start()

    loop(6, input_back, planned("inb"))
    planned("tail")
    for i in range(6):
        put_hidden(i).wait()


def emit_kernel(*refs):
    hidden, shards, gvec, loss = refs[0], refs[1:7], refs[7], refs[8]
    hidden_o, shards_o, vectors_o, loss_o = refs[9], refs[10:16], refs[16:25], refs[25]
    held, parts, sem_in, sem_out = refs[26], refs[27:33], refs[33], refs[34]
    moves = [
        (hidden.at[block(k, 128), :], held.at[block(k, 128), :], hidden_o.at[block(k, 128), :])
        for k in range(8)
    ] + list(zip(shards, parts, shards_o))
    for k, (src, mid, _) in enumerate(moves):
        pltpu.make_async_copy(src, mid, sem_in.at[k]).start()
    for k, size in enumerate(VECTOR_SIZES):
        vectors_o[k][...] = gvec[k, 0:size]
    loss_o[0] = loss[0, 0]
    for k, (src, mid, dst) in enumerate(moves):
        pltpu.make_async_copy(src, mid, sem_in.at[k]).wait()
        pltpu.make_async_copy(mid, dst, sem_out.at[k]).start()
    for k, (_, mid, dst) in enumerate(moves):
        pltpu.make_async_copy(mid, dst, sem_out.at[k]).wait()


def fused_device(hidden_in, seq_lengths, pos_index, pos_count, *masters):
    x = hidden_in.reshape(TOK, WIDTH)
    whole = pl.BlockSpec(memory_space=pltpu.VMEM)
    scalars = pl.BlockSpec(memory_space=pltpu.SMEM)
    away = pl.BlockSpec(memory_space=pl.ANY)
    shape = jax.ShapeDtypeStruct
    square = shape((24, 768), F32)
    shards = [square] * 4 + [shape((24, 3072), F32), shape((96, 768), F32)]
    pieces = len(PIECES)
    outs = pl.pallas_call(
        step_kernel,
        out_shape=[
            shape((1, 1), F32),
            shape((TOK, WIDTH), F32),
            shape((12, 2, SENT, SENT), BF),
            *shards,
            shape((16, 128), F32),
        ],
        in_specs=[scalars, away, whole, whole] + [away] * 6 + [whole] * 9,
        out_specs=[whole, away, away] + [whole] * 7,
        scratch_shapes=[
            pltpu.VMEM((WIDTH, INNER), BF),
            pltpu.VMEM((WIDTH, INNER), BF),
            pltpu.VMEM((INNER, WIDTH), BF),
            pltpu.VMEM((512, 128), F32),
            pltpu.VMEM((INNER, WIDTH), BF),
            pltpu.VMEM((SLOTS, 384, 768), BF),
            pltpu.VMEM((SLOTS, 2, 96, 384), BF),
            pltpu.VMEM((SLOTS, 2, 96, 768), BF),
            pltpu.VMEM((SLOTS, 3, 24, 768), BF),
            pltpu.VMEM((TOK, INNER), BF),
            pltpu.VMEM((TOK, INNER), BF),
            pltpu.VMEM((TOK, 2304), BF),
            pltpu.VMEM((TOK, WIDTH), BF),
            pltpu.VMEM((TOK, WIDTH), BF),
            pltpu.VMEM((TOK, WIDTH), BF),
            pltpu.VMEM((TOK, WIDTH), BF),
            pltpu.VMEM((TOK, WIDTH), F32),
            pltpu.VMEM((2, 2, SENT, SENT), BF),
            pltpu.VMEM((TOK, 1), F32),
            pltpu.VMEM((TOK, 1), F32),
            pltpu.VMEM((16, INNER), F32),
            pltpu.VMEM((16, INNER), F32),
            pltpu.VMEM((8, WIDTH), F32),
            pltpu.VMEM((8, WIDTH), F32),
            pltpu.VMEM((512, 128), BF),
            pltpu.VMEM((256, 128), F32),
            pltpu.VMEM((2, 32, 128), F32),
            pltpu.VMEM((2, 64, 128), F32),
            pltpu.VMEM((3, 16, 128), F32),
            pltpu.SemaphoreType.DMA((pieces, 6)),
            pltpu.SemaphoreType.DMA((pieces,)),
            pltpu.SemaphoreType.DMA((VEC + 1, 6)),
            pltpu.SemaphoreType.DMA((VEC + 1, 2)),
            pltpu.SemaphoreType.REGULAR((SLOTS,)),
            pltpu.SemaphoreType.DMA,
            pltpu.SemaphoreType.DMA,
            pltpu.SemaphoreType.DMA((2,)),
            pltpu.SemaphoreType.DMA((6,)),
            pltpu.SemaphoreType.DMA((10,)),
            pltpu.VMEM((TOK, WIDTH), BF),
        ],
        compiler_params=pltpu.CompilerParams(
            collective_id=0, has_side_effects=True, vmem_limit_bytes=VMEM_ALL
        ),
        name="train_step",
    )(seq_lengths.reshape(2), x, jnp.transpose(pos_index, (2, 0, 1)), pos_count, *masters)
    loss, hidden, grads = outs[0], outs[1], outs[3:]
    vectors = [shape((size,), F32) for size in VECTOR_SIZES]
    final = pl.pallas_call(
        emit_kernel,
        out_shape=[shape((TOK, WIDTH), F32), *shards, *vectors, shape((1,), F32)],
        in_specs=[away] * 7 + [whole, scalars],
        out_specs=[away] * 7 + [whole] * 9 + [scalars],
        scratch_shapes=[pltpu.VMEM((TOK, WIDTH), F32)]
        + [pltpu.VMEM(s.shape, F32) for s in shards]
        + [pltpu.SemaphoreType.DMA((14,)), pltpu.SemaphoreType.DMA((14,))],
        name="emit",
    )(hidden, *grads[:6], grads[6], loss)
    return (final[16].reshape(()), final[0].reshape(hidden_in.shape), *final[1:16])


def device_step(mesh):
    if mesh.shape["twin"] == 2 and mesh.shape["dp"] == 16:
        return fused_device
    return staged_device


def solution(mesh):
    in_specs = (
        P("twin", "dp", None, None),
        P("twin", "dp"),
        P(),
        P(),
        P(("twin", "dp"), None),
        P(("twin", "dp"), None),
        P(("twin", "dp"), None),
        P(("twin", "dp"), None),
        P(("twin", "dp"), None),
        P(("twin", "dp"), None),
        P(("twin", "dp")),
        P(("twin", "dp")),
        P(("twin", "dp")),
        P(("twin", "dp")),
        P(("twin", "dp")),
        P(("twin", "dp")),
        P(("twin", "dp")),
        P(("twin", "dp")),
        P(("twin", "dp")),
    )
    out_specs = (
        P(),
        P("twin", "dp", None, None),
        P(("twin", "dp"), None),
        P(("twin", "dp"), None),
        P(("twin", "dp"), None),
        P(("twin", "dp"), None),
        P(("twin", "dp"), None),
        P(("twin", "dp"), None),
        P(("twin", "dp")),
        P(("twin", "dp")),
        P(("twin", "dp")),
        P(("twin", "dp")),
        P(("twin", "dp")),
        P(("twin", "dp")),
        P(("twin", "dp")),
        P(("twin", "dp")),
        P(("twin", "dp")),
    )
    return jax.shard_map(
        device_step(mesh), mesh=mesh, in_specs=in_specs, out_specs=out_specs, check_vma=False
    )
```
